32 devices in a mesh: groups: 2 (over x), kvseq: 8 (over z, y), tensor: 2 (over core).
Axes of the slice: x: 2, y: 2, z: 4, core: 2. Of those that a mesh axis runs over, the one named last changes fastest.
Arguments:
- hidden: bfloat16 [16, 8192], P('groups', 'kvseq'), parts along dimension 0, may hold values from -30 to 30
- lengths: int32 [16], P('groups'), parts along dimension 0, may hold values from 128 to 2048, as said below
- key_cache: bfloat16 [16, 2048, 1024], P('groups', 'kvseq', 'tensor'), parts along dimension 0, may hold values from -400 to 400
- value_cache: bfloat16 [16, 2048, 1024], P('groups', 'kvseq', 'tensor'), parts along dimension 0, may hold values from -60 to 60
- gain_in: float32 [8192], P('kvseq'), may hold values from 0.1 to 1.9
- w_query: bfloat16 [8192, 8192], P('kvseq', 'tensor'), may hold values from -0.0625 to 0.0625
- w_key: bfloat16 [8192, 1024], P('kvseq', 'tensor'), may hold values from -0.0625 to 0.0625
- w_value: bfloat16 [8192, 1024], P('kvseq', 'tensor'), may hold values from -0.0625 to 0.0625
- w_output: bfloat16 [8192, 8192], P('tensor', 'kvseq'), may hold values from -0.0625 to 0.0625
- gain_post: float32 [8192], P('kvseq'), may hold values from 0.1 to 1.9
- w_gate: bfloat16 [8192, 15360], P('kvseq', 'tensor'), may hold values from -0.0625 to 0.0625
- w_up: bfloat16 [8192, 15360], P('kvseq', 'tensor'), may hold values from -0.0625 to 0.0625
- w_down: bfloat16 [15360, 8192], P('tensor', 'kvseq'), may hold values from -0.046875 to 0.046875
Outputs:
- output: bfloat16 [16, 8192], P('groups', 'kvseq'), parts along dimension 0
- new_keys: bfloat16 [16, 1024], P('groups', 'tensor'), parts along dimension 0
- new_values: bfloat16 [16, 1024], P('groups', 'tensor'), parts along dimension 0
The draws below stay inside these ranges and needn't reach their ends.
There are 2 independent parts, one for each index of `groups`. The reference program is written for one: setup_inputs(seed, part) draws one part's arguments, and reference() takes and returns one part's arrays. A program takes and returns all parts, laid end to end along the dimension named above; an argument that names none is the same for every part. Nothing has to cross between parts.
Inputs may be any that keep to these rules, and one draw needn't show every extreme that they name: `lengths`: multiples of 128; some sequence holds exactly 2048.
All inputs are finite; a program needn't handle non-finite values.
Results may differ from the reference program's by a relative error of at most 0.024.
Values may be sent and summed in bfloat16 or wider, within the bound.
A program may use at most 128 MiB of HBM per device.

```python
import jax
import jax.numpy as jnp
from jax import lax

D = 8192
H = 64
KVH = 8
HD = 128
FF = 15360
SEQS = 8
PAGE = 128
LENGTH = 2048


def draw_hidden(key, part):
    ramp = jnp.exp(jnp.linspace(0.0, jnp.log(3.0), D)).astype(jnp.float32)
    rough = jax.random.uniform(jax.random.fold_in(key, 11), (D,), jnp.float32, 0.5, 1.5)
    base = jnp.clip(jax.random.normal(jax.random.fold_in(key, 12), (SEQS, D), jnp.float32), -6.0, 6.0)
    return (base * ramp * rough).astype(jnp.bfloat16)


def draw_lengths(key, part):
    pages = jax.random.randint(jax.random.fold_in(key, 21), (SEQS,), 1, LENGTH // PAGE + 1) * PAGE
    chosen = jax.random.randint(jax.random.fold_in(key, 22), (), 0, SEQS)
    return pages.at[chosen].set(LENGTH).astype(jnp.int32)


def draw_key_cache(key, part):
    base = jnp.clip(jax.random.normal(jax.random.fold_in(key, 31), (SEQS, LENGTH, KVH * HD), jnp.float32), -6.0, 6.0)
    return base.astype(jnp.bfloat16)


def draw_value_cache(key, part):
    place = jnp.arange(LENGTH, dtype=jnp.float32) / LENGTH
    magnitude = jax.random.uniform(jax.random.fold_in(key, 41), (KVH * HD,), jnp.float32, 0.5, 1.5)
    sign = jnp.where(jax.random.bernoulli(jax.random.fold_in(key, 42), 0.5, (KVH * HD,)), 1.0, -1.0)
    common = 1.5 * magnitude * sign
    ramp = jnp.exp(place * jnp.log(4.0))
    rough = jnp.clip(jax.random.normal(jax.random.fold_in(key, 43), (SEQS, LENGTH, KVH * HD), jnp.float32), -3.0, 3.0)
    values = (rough + common[None, None, :]) * ramp[None, :, None]
    return values.astype(jnp.bfloat16)


def shard_levels(rng, extent, shards, least, high):
    level = 1.0
    for dim, parts in shards:
        draws = jax.random.uniform(jax.random.fold_in(jax.random.fold_in(rng, 6), dim), (parts,), jnp.float32, least / len(shards), high / len(shards))
        level = level * jnp.repeat(jnp.exp(draws), extent[dim] // parts).reshape((-1,) + (1,) * (len(extent) - 1 - dim))
    return level


def bell_draw(rng, shape, spread, limit, split=(), kind=jnp.bfloat16):
    drawn = spread * jax.random.normal(rng, shape, jnp.float32)
    if split:
        drawn = drawn * shard_levels(rng, shape, split, -0.22, 0.18)
    return jnp.clip(drawn, -limit, limit).astype(kind)


def setup_inputs(seed: int = 0, part: int = 0) -> dict:
    key_list = jax.random.split(jax.random.key(seed), 14)
    part_splits = jax.random.split(jax.random.fold_in(key_list[13], part), 14)
    hidden = draw_hidden(jax.random.fold_in(jax.random.fold_in(key_list[13], part), 71), part)
    lengths = draw_lengths(jax.random.fold_in(jax.random.fold_in(key_list[13], part), 71), part)
    key_cache = draw_key_cache(jax.random.fold_in(jax.random.fold_in(key_list[13], part), 71), part)
    value_cache = draw_value_cache(jax.random.fold_in(jax.random.fold_in(key_list[13], part), 71), part)
    gain_in = jnp.clip(1.0 + 0.18 * jax.random.normal(key_list[4], (D,), jnp.float32), 0.1, 1.9)
    w_query = bell_draw(key_list[5], (D, H * HD), D ** -0.5, 0.0625, ((0, 8), (1, 2)))
    w_key = bell_draw(key_list[6], (D, KVH * HD), D ** -0.5, 0.0625, ((0, 8), (1, 2)))
    w_value = bell_draw(key_list[7], (D, KVH * HD), D ** -0.5, 0.0625, ((0, 8), (1, 2)))
    w_output = bell_draw(key_list[8], (H * HD, D), (H * HD) ** -0.5, 0.0625, ((0, 2), (1, 8)))
    gain_post = jnp.clip(1.0 + 0.18 * jax.random.normal(key_list[9], (D,), jnp.float32), 0.1, 1.9)
    w_gate = bell_draw(key_list[10], (D, FF), D ** -0.5, 0.0625, ((0, 8), (1, 2)))
    w_up = bell_draw(key_list[11], (D, FF), D ** -0.5, 0.0625, ((0, 8), (1, 2)))
    w_down = bell_draw(key_list[12], (FF, D), FF ** -0.5, 0.046875, ((0, 2), (1, 8)))
    return dict(hidden=hidden, lengths=lengths, key_cache=key_cache, value_cache=value_cache, gain_in=gain_in, w_query=w_query, w_key=w_key, w_value=w_value, w_output=w_output, gain_post=gain_post, w_gate=w_gate, w_up=w_up, w_down=w_down)


epsilon = 1e-06
rope_base = 1000000.0

def rotate(values, position):
    half_dim = values.shape[-1] // 2
    frequency = rope_base ** (-jnp.arange(half_dim, dtype=jnp.float32) * 2.0 / values.shape[-1])
    angles = position[:, None, None] * frequency
    cosine = jnp.cos(angles)
    sine = jnp.sin(angles)
    lower = values[..., :half_dim]
    upper = values[..., half_dim:]
    return jnp.concatenate([lower * cosine - upper * sine, upper * cosine + lower * sine], axis=-1)

def rms_norm(stream, gain):
    scale = lax.rsqrt(lax.optimization_barrier(jnp.mean(stream * stream, axis=1, keepdims=True)) + epsilon)
    return (stream * scale * gain).astype(jnp.bfloat16)

def reference(hidden, lengths, key_cache, value_cache, gain_in, w_query, w_key, w_value, w_output, gain_post, w_gate, w_up, w_down):
    stream = hidden.astype(jnp.float32)
    normed = rms_norm(stream, gain_in)
    query = jnp.dot(normed, w_query, preferred_element_type=jnp.float32)
    key = jnp.dot(normed, w_key, preferred_element_type=jnp.float32)
    value = jnp.dot(normed, w_value, preferred_element_type=jnp.float32)
    position = lengths.astype(jnp.float32)
    query = rotate(query.reshape(SEQS, H, HD), position)
    new_keys = rotate(key.reshape(SEQS, KVH, HD), position).astype(jnp.bfloat16)
    new_values = value.reshape(SEQS, KVH, HD).astype(jnp.bfloat16)
    grouped = query.astype(jnp.bfloat16).reshape(SEQS, KVH, H // KVH, HD).astype(jnp.float32)
    cached_keys = key_cache.reshape(SEQS, LENGTH, KVH, HD).astype(jnp.float32)
    cached_values = value_cache.reshape(SEQS, LENGTH, KVH, HD).astype(jnp.float32)
    factor = float(HD) ** (-0.5)
    scores = jnp.einsum('skgd,slkd->skgl', grouped, cached_keys) * factor
    valid = (jnp.arange(LENGTH, dtype=jnp.int32)[None, :] < lengths[:, None])[:, None, None, :]
    masked = jnp.where(valid, scores, -1e+30)
    own = jnp.einsum('skgd,skd->skg', grouped, new_keys.astype(jnp.float32)) * factor
    top = jnp.maximum(lax.optimization_barrier(jnp.max(masked, axis=-1)), own)
    weights = jnp.where(valid, jnp.exp(masked - top[..., None]), 0.0)
    own_weight = jnp.exp(own - top)
    total = lax.optimization_barrier(jnp.sum(weights, axis=-1)) + own_weight
    mixed = jnp.einsum('skgl,slkd->skgd', weights.astype(jnp.bfloat16).astype(jnp.float32), cached_values)
    mixed = mixed + own_weight[..., None] * new_values.astype(jnp.float32)[:, :, None, :]
    attended = (mixed / total[..., None]).astype(jnp.bfloat16).reshape(SEQS, H * HD)
    residual = stream + jnp.dot(attended, w_output, preferred_element_type=jnp.float32)
    normed_post = rms_norm(residual, gain_post)
    gate = jnp.dot(normed_post, w_gate, preferred_element_type=jnp.float32)
    upward = jnp.dot(normed_post, w_up, preferred_element_type=jnp.float32)
    inner = (jax.nn.silu(gate) * upward).astype(jnp.bfloat16)
    output = (residual + jnp.dot(inner, w_down, preferred_element_type=jnp.float32)).astype(jnp.bfloat16)
    return (output, new_keys.reshape(SEQS, KVH * HD), new_values.reshape(SEQS, KVH * HD))
```

```python
import functools

import jax
import jax.numpy as jnp
import numpy as np
from jax import lax
from jax.experimental import pallas as pl
from jax.experimental.pallas import tpu as pltpu
from jax.sharding import PartitionSpec as P

HD = 128
epsilon = 1e-06
rope_base = 1000000.0
BF = jnp.bfloat16
F32 = jnp.float32
MESH = pl.DeviceIdType.MESH


def mult(x, m):
    return pl.multiple_of(x, m)


def accumulate(n, load, op=jnp.add):
    u = 8 if n % 8 == 0 else 1

    def group(first, acc):
        for j in range(u):
            x = load(first + j)
            acc = x if acc is None else jax.tree.map(op, acc, x)
        return acc

    acc = group(0, None)
    if n == u:
        return acc
    return lax.fori_loop(1, n // u, lambda i, a: group(i * u, a), acc)


def split_kernel(packed, out, new_keys, new_values):
    Dl, KC = out.shape[1], new_keys.shape[1]
    out[...] = packed[:, :Dl]
    new_keys[...] = packed[:, Dl : Dl + KC]
    new_values[...] = packed[:, Dl + KC :]


def layer_kernel(
    c,
    lengths_hbm,
    hidden_hbm,
    gain_in_hbm,
    gain_post_hbm,
    freq_hbm,
    kc_hbm,
    vc_hbm,
    wq_hbm,
    wk_hbm,
    wv_hbm,
    wo_hbm,
    wg_hbm,
    wu_hbm,
    wd_hbm,
    out,
    lengths,
    hidden,
    gain_in,
    gain_post,
    freq,
    wqkv,
    tail,
    wo,
    wg,
    wu,
    kc,
    vc,
    send_a,
    recv_a,
    qg,
    kvg,
    own_scores,
    all_q,
    all_kv,
    send_b,
    recv_b,
    ab,
    all_b,
    part_1,
    send_c0,
    send_c1,
    recv_c0,
    recv_c1,
    ic0,
    ic1,
    all_c0,
    all_c1,
    part_2,
    ssem,
    wsem,
    fsem,
    dsem,
    sa_s,
    sa_r,
    ga_s,
    ga_r,
    gk_s,
    gk_r,
    sb_s,
    sb_r,
    gb_s,
    gb_r,
    t1_s,
    t1_r,
    sc_s,
    sc_r,
    gc_s,
    gc_r,
    t2_s,
    t2_r,
):
    n, T, O = c["n"], c["T"], c["O"]
    S, Dl, L = c["S"], c["Dl"], c["L"]
    PG, FO, F0, F1 = c["PG"], c["FO"], c["F0"], c["F1"]
    QG = PG * HD
    G3 = QG + 2 * HD
    KC = O * HD
    W0, W1 = F0 * HD, F1 * HD
    D = float(Dl * n)
    base = (n - O) // 2
    me = lax.axis_index("kvseq")
    t = lax.axis_index("tensor")
    owner = (me >= base) & (me < base + O) & (t == T - 1)
    o_me = me - base
    half_n = n // 2
    side = me // half_n

    def mine(o):
        return (me == base + o) & (t == T - 1)

    def order(k):
        if O != 4:
            return lax.rem(me + k, O)
        oz = (side + 1 + k // 2) % 2
        oy = (me + 1 + k % 2) % 2
        return oz * 2 + oy

    def near(k):
        return order(O - 1 - k)

    def local(src, dst, sem):
        return pltpu.make_async_copy(src, dst, sem)

    small = [
        local(hidden_hbm, hidden, ssem.at[0]),
        local(gain_in_hbm, gain_in, ssem.at[1]),
        local(lengths_hbm, lengths, ssem.at[2]),
        local(freq_hbm, freq, ssem.at[3]),
        local(gain_post_hbm, gain_post, ssem.at[4]),
    ]
    half = Dl // 2

    def first(k):
        o = order(k)
        return [
            [
                local(
                    src.at[pl.ds(b * half, half), pl.ds(mult(o * width, HD), width)],
                    wqkv.at[k, pl.ds(b * half, half), pl.ds(at, width)],
                    fsem.at[k, b, i],
                )
                for i, (src, at, width) in enumerate(
                    ((wq_hbm, 0, QG), (wk_hbm, QG, HD), (wv_hbm, QG + HD, HD))
                )
            ]
            for b in range(2)
        ]

    firsts = [first(k) for k in range(O)]
    kv_copies = [local(kc_hbm, kc, wsem.at[0]), local(vc_hbm, vc, wsem.at[1])]
    later = [
        local(wo_hbm, wo, wsem.at[2]),
        local(wg_hbm, wg, wsem.at[3]),
        local(wu_hbm, wu, wsem.at[4]),
    ]

    def down_0(o):
        return wo.at[pl.ds(mult(o * QG, HD), W0), :]

    def down_1(o):
        return wqkv.at[o, pl.ds(0, W1), pl.ds(0, Dl)] if c["reuse"] else tail.at[o]

    downs_0 = [
        local(wd_hbm.at[pl.ds(o * FO * HD, W0), :], down_0(o), dsem.at[0, o]) for o in range(O)
    ]
    downs_1 = [
        local(wd_hbm.at[pl.ds((o * FO + F0) * HD, W1), :], down_1(o), dsem.at[1, o])
        for o in range(O)
    ]
    for x in small:
        x.start()
    for k in range(O):
        for b in range(2):
            for x in firsts[k][b]:
                x.start(priority=1)

    barrier = pltpu.get_barrier_semaphore()
    for dt in range(T):

        def greet(k, _):
            pl.semaphore_signal(
                barrier,
                inc=1,
                device_id={"kvseq": lax.rem(me + k, n), "tensor": lax.rem(t + dt, T)},
                device_id_type=MESH,
            )
            return 0

        lax.fori_loop(0 if dt else 1, n, greet, 0)

    def remote(src, dst, s_sem, r_sem, k, tt):
        return pltpu.make_async_remote_copy(
            src_ref=src, dst_ref=dst, send_sem=s_sem, recv_sem=r_sem,
            device_id={"kvseq": k, "tensor": tt}, device_id_type=MESH,
        )

    def to_owner(src, recv, s_sem, r_sem, o):
        return remote(src, recv, s_sem, r_sem, base + o, T - 1)

    def scatter(src, dst, s_sem, r_sem, o):
        @pl.when(jnp.logical_not(mine(o)))
        def _():
            to_owner(src, dst, s_sem, r_sem, o).start()

        @pl.when(mine(o))
        def _():
            dst[...] = src[...]

    def scatter_wait_send(src, dst, s_sem, r_sem, o):
        @pl.when(jnp.logical_not(mine(o)))
        def _():
            to_owner(src, dst, s_sem, r_sem, o).wait_send()

    def owner_wait(recv, s_sem, r_sem, tt):
        def one(k, _):
            def wait():
                remote(recv(k), recv(k), s_sem, r_sem(k), k, tt).wait_recv()

            if tt == T - 1:
                pl.when(k != me)(wait)
            else:
                wait()
            return 0

        lax.fori_loop(0, n, one, 0)

    def each_target(f):
        def cross(k, _):
            f(k + (1 - side) * (n - 1 - 2 * k))
            return 0

        def same(k, _):
            f(k + side * (n - 1 - 2 * k))
            return 0

        lax.fori_loop(0, half_n, cross, 0)
        lax.fori_loop(0, n - half_n, same, 0)

    def spread(src, dst, s_sem, r_sem, tt):
        def one(d):
            def send():
                remote(src, dst, s_sem.at[tt, d], r_sem, d, tt).start()

            if tt == T - 1:
                pl.when(d != me)(send)
            else:
                send()

        each_target(one)
        if tt == T - 1:
            dst[...] = src[...]

    def spread_wait_send(src, dst, s_sem, r_sem, tt):
        def one(d, _):
            def wait():
                remote(src, dst, s_sem.at[tt, d], r_sem, d, tt).wait_send()

            if tt == T - 1:
                pl.when(d != me)(wait)
            else:
                wait()
            return 0

        lax.fori_loop(0, n, one, 0)

    def spread_wait(dst, s_sem, r_sem, o):
        @pl.when(jnp.logical_not(mine(o)))
        def _():
            remote(dst, dst, s_sem.at[0, 0], r_sem, base + o, T - 1).wait_recv()

    def pair_copies(part, s_sem, r_sem):
        return [
            remote(part.at[t], part.at[t], s_sem.at[k], r_sem.at[t], me, lax.rem(t + k, T))
            for k in range(1, T)
        ]

    def pair_sum(part, s_sem, r_sem):
        for x in pair_copies(part, s_sem, r_sem):
            x.start()
        for k in range(1, T):
            src = lax.rem(t + k, T)
            remote(part.at[src], part.at[src], s_sem.at[k], r_sem.at[src], me, src).wait_recv()
        total = part[0]
        for i in range(1, T):
            total = total + part[i]
        return total

    lane = lax.broadcasted_iota(jnp.int32, (S, HD), 1)
    row = lax.broadcasted_iota(jnp.int32, (S, HD), 0)

    def squares_block(x):
        s = jnp.broadcast_to(jnp.sum(x * x, axis=1, keepdims=True), (S, HD))
        high = s.astype(BF).astype(F32)
        return jnp.where(lane < HD // 2, high, s - high).astype(BF)

    def row_scale(block):
        total = jnp.sum(block, axis=1, keepdims=True) * (2.0 / HD)
        return lax.rsqrt(total / D + epsilon)

    small[0].wait()
    small[1].wait()
    stream = hidden[...].astype(F32)
    xg = (stream * gain_in[...]).astype(BF)
    sq = squares_block(stream)

    for k in range(O):
        o = order(k)
        for x in firsts[k][0]:
            x.wait()
        part = jnp.dot(xg[:, :half], wqkv[k, :half, :], preferred_element_type=F32)
        for x in firsts[k][1]:
            x.wait()
        if k == max(O - 2, 0):
            for x in kv_copies:
                x.start(priority=1)
        part = part + jnp.dot(xg[:, half:], wqkv[k, half:, :], preferred_element_type=F32)
        send_a[k, :, :G3] = part.astype(BF)
        send_a[k, :, G3:] = sq
        if k == 0:
            pl.semaphore_wait(barrier, n * T - 1)
        scatter(send_a.at[k], recv_a.at[t, me], sa_s.at[k], sa_r.at[t, me], o)
    for x in later + downs_1:
        x.start(priority=1)

    small[2].wait()
    small[3].wait()
    position = jnp.zeros((S, HD), F32)
    for s in range(S):
        position = jnp.where(row == s, lengths[s].astype(F32), position)
    angle = position * freq[...]
    cosine = jnp.cos(angle)
    sine = jnp.sin(angle)
    sine = jnp.where(lane < HD // 2, -sine, sine)
    factor = float(HD) ** (-0.5)

    @pl.when(owner)
    def _():
        for tt in reversed(range(T)):
            owner_wait(lambda k: recv_a.at[tt, k], sa_s.at[0], lambda k: sa_r.at[tt, k], tt)
            total = accumulate(n, lambda k: recv_a[tt, k].astype(F32))
            scale = row_scale(total[:, G3:])
            for j in range(PG + 1):
                v = total[:, j * HD : (j + 1) * HD] * scale
                v = (v * cosine + pltpu.roll(v, HD // 2, 1) * sine).astype(BF)
                if j < PG:
                    qg[tt, :, j * HD : (j + 1) * HD] = v
                else:
                    kvg[tt, :, :HD] = v
            kvg[tt, :, HD:] = (total[:, QG + HD : G3] * scale).astype(BF)
            spread(qg.at[tt], all_q.at[o_me], ga_s, ga_r.at[o_me], tt)
        for tt in range(T):
            spread(kvg.at[tt], all_kv.at[o_me], gk_s, gk_r.at[o_me], tt)
        for tt in range(T):
            key = kvg[tt, :, :HD].astype(F32)
            block = jnp.zeros((S, HD), F32)
            for j in range(PG):
                q = qg[tt, :, j * HD : (j + 1) * HD].astype(F32)
                block = jnp.where(
                    lane == j, jnp.sum(q * key, axis=1, keepdims=True) * factor, block
                )
            own_scores[tt] = block

    R = PG * S
    brow = lax.broadcasted_iota(jnp.int32, (R, L), 0) % S
    orow = lax.broadcasted_iota(jnp.int32, (R, HD), 0) % S
    limit = jnp.zeros((R, L), jnp.int32)
    for s in range(S):
        limit = jnp.where(brow == s, lengths[s], limit)
    place = lax.broadcasted_iota(jnp.int32, (R, L), 1) + me * L
    valid = place < limit
    for x in kv_copies:
        x.wait()
    group = lane % 16
    third = (lane % (HD // 2)) // 16

    def attend(i, _):
        g = near(i)
        spread_wait(all_q.at[g], ga_s, ga_r.at[g], g)
        q = jnp.concatenate(
            [all_q[g, :, j * HD : (j + 1) * HD].astype(F32) for j in range(PG)], axis=0
        ).astype(BF)
        cols = pl.ds(mult(g * HD, HD), HD)
        scores = jnp.zeros((R, L), F32)
        for s in range(S):
            x = lax.dot_general(
                q, kc[s, :, cols], (((1,), (1,)), ((), ())), preferred_element_type=F32
            )
            scores = jnp.where(brow == s, x, scores)
        scores = jnp.where(valid, scores * factor, -1e30)
        top = jnp.max(scores, axis=1, keepdims=True)
        w = jnp.where(valid, jnp.exp(scores - top), 0.0)
        total = jnp.sum(w, axis=1, keepdims=True)
        w = w.astype(BF)
        mixed = jnp.zeros((R, HD), F32)
        for s in range(S):
            x = jnp.dot(w, vc[s, :, cols], preferred_element_type=F32)
            mixed = jnp.where(orow == s, x, mixed)
        ml = jnp.zeros((S, HD), F32)
        for j in range(PG):
            rows = slice(j * S, (j + 1) * S)
            send_b[g, :, j * HD : (j + 1) * HD] = mixed[rows].astype(BF)
            ml = jnp.where(group == j, jnp.where(lane < HD // 2, top[rows], total[rows]), ml)
        high = ml.astype(BF).astype(F32)
        rest = ml - high
        middle = rest.astype(BF).astype(F32)
        low = rest - middle
        parts = jnp.where(third == 0, high, jnp.where(third == 1, middle, low))
        send_b[g, :, QG:] = parts.astype(BF)
        scatter(send_b.at[g], recv_b.at[t, me], sb_s.at[g], sb_r.at[t, me], g)
        return 0

    lax.fori_loop(0, O, attend, 0)

    @pl.when(owner)
    def _():
        for tt in reversed(range(T)):
            owner_wait(lambda k: recv_b.at[tt, k], sb_s.at[0], lambda k: sb_r.at[tt, k], tt)

            def stats(k):
                x = recv_b[tt, k, :, QG:].astype(F32)
                return x + pltpu.roll(x, HD - 16, 1) + pltpu.roll(x, HD - 32, 1)

            top = accumulate(n, stats, jnp.maximum)
            total = accumulate(
                n, lambda k: pltpu.roll(stats(k), HD // 2, 1) * jnp.exp(stats(k) - top)
            )
            own = own_scores[tt]
            best = jnp.maximum(top, own)
            old_scale = jnp.exp(top - best)
            own_weight = jnp.exp(own - best)
            bottom = total * old_scale + own_weight
            old_scale = old_scale / bottom
            own_weight = own_weight / bottom

            def weighted(k):
                scale = jnp.exp(stats(k) - top) * old_scale
                return tuple(
                    recv_b[tt, k, :, j * HD : (j + 1) * HD].astype(F32) * scale[:, j : j + 1]
                    for j in range(PG)
                )

            mixed = accumulate(n, weighted)
            val = kvg[tt, :, HD:].astype(F32)
            for j in range(PG):
                res = mixed[j] + own_weight[:, j : j + 1] * val
                ab[tt, :, j * HD : (j + 1) * HD] = res.astype(BF)
            spread(ab.at[tt], all_b.at[o_me], gb_s, gb_r.at[o_me], tt)

    later[0].wait()

    def output_block(i, acc):
        g = near(i)
        spread_wait(all_b.at[g], gb_s, gb_r.at[g], g)
        w = wo[pl.ds(mult(g * QG, HD), QG), :]
        return acc + jnp.dot(all_b[g], w, preferred_element_type=F32)

    part_1[t] = lax.fori_loop(0, O, output_block, jnp.zeros((S, Dl), F32))
    for x in downs_0:
        x.start(priority=1)
    small[4].wait()
    residual = hidden[...].astype(F32) + pair_sum(part_1, t1_s, t1_r)
    sq_post = squares_block(residual)
    rg = (residual * gain_post[...]).astype(BF)
    later[1].wait()
    later[2].wait()

    def widen(k, _):
        o = order(k)
        for send, recv, i, at, W in (
            (send_c0, recv_c0, 0, 0, W0),
            (send_c1, recv_c1, 1, F0, W1),
        ):
            begin = (o * FO + at) * HD
            for b, w in enumerate((wg, wu)):
                for j in range(0, W, 256):
                    step = min(256, W - j)
                    x = jnp.dot(
                        rg, w[:, pl.ds(mult(begin + j, HD), step)], preferred_element_type=F32
                    )
                    send[o, :, b * W + j : b * W + j + step] = x.astype(BF)
            if i == 0:
                send[o, :, 2 * W :] = sq_post
            scatter(send.at[o], recv.at[t, me], sc_s.at[o, i], sc_r.at[t, me, i], o)
        return 0

    lax.fori_loop(0, O, widen, 0)

    for g in range(O):
        spread_wait(all_kv.at[g], gk_s, gk_r.at[g], g)
        out[:, Dl + g * HD : Dl + (g + 1) * HD] = all_kv[g, :, :HD]
        out[:, Dl + KC + g * HD : Dl + KC + (g + 1) * HD] = all_kv[g, :, HD:]

    @pl.when(owner)
    def _():
        scales = [None] * T
        for i, recv, ic, all_c, W in ((0, recv_c0, ic0, all_c0, W0), (1, recv_c1, ic1, all_c1, W1)):
            for tt in reversed(range(T)):
                owner_wait(
                    lambda k: recv.at[tt, k], sc_s.at[0, 0], lambda k: sc_r.at[tt, k, i], tt
                )
                if i == 0:
                    scales[tt] = row_scale(
                        accumulate(n, lambda k: recv[tt, k, :, 2 * W :].astype(F32))
                    )
                for j in range(0, W, HD):
                    gate = accumulate(n, lambda k: recv[tt, k, :, j : j + HD].astype(F32))
                    up = accumulate(n, lambda k: recv[tt, k, :, W + j : W + j + HD].astype(F32))
                    gate = gate * scales[tt]
                    up = up * scales[tt]
                    ic[tt, :, j : j + HD] = (gate * jax.nn.sigmoid(gate) * up).astype(BF)
                spread(ic.at[tt], all_c.at[o_me], gc_s.at[i], gc_r.at[o_me, i], tt)

    for x in downs_0 + downs_1:
        x.wait()

    def down_block(k, acc):
        o = near(k)
        spread_wait(all_c0.at[o], gc_s.at[0], gc_r.at[o, 0], o)
        acc = acc + jnp.dot(all_c0[o], down_0(o)[...], preferred_element_type=F32)
        spread_wait(all_c1.at[o], gc_s.at[1], gc_r.at[o, 1], o)
        return acc + jnp.dot(all_c1[o], down_1(o)[...], preferred_element_type=F32)

    part_2[t] = lax.fori_loop(0, O, down_block, jnp.zeros((S, Dl), F32))
    out[:, :Dl] = (residual + pair_sum(part_2, t2_s, t2_r)).astype(BF)

    for k in range(O):
        scatter_wait_send(send_a.at[k], recv_a.at[t, me], sa_s.at[k], sa_r.at[t, me], order(k))

    def sent(o, _):
        scatter_wait_send(send_b.at[o], recv_b.at[t, me], sb_s.at[o], sb_r.at[t, me], o)
        for i, send, recv in ((0, send_c0, recv_c0), (1, send_c1, recv_c1)):
            scatter_wait_send(
                send.at[o], recv.at[t, me], sc_s.at[o, i], sc_r.at[t, me, i], o
            )
        return 0

    lax.fori_loop(0, O, sent, 0)

    @pl.when(owner)
    def _():
        for tt in range(T):
            spread_wait_send(qg.at[tt], all_q.at[o_me], ga_s, ga_r.at[o_me], tt)
            spread_wait_send(kvg.at[tt], all_kv.at[o_me], gk_s, gk_r.at[o_me], tt)
            spread_wait_send(ab.at[tt], all_b.at[o_me], gb_s, gb_r.at[o_me], tt)
            spread_wait_send(ic0.at[tt], all_c0.at[o_me], gc_s.at[0], gc_r.at[o_me, 0], tt)
            spread_wait_send(ic1.at[tt], all_c1.at[o_me], gc_s.at[1], gc_r.at[o_me, 1], tt)

    for part, s_sem, r_sem in ((part_1, t1_s, t1_r), (part_2, t2_s, t2_r)):
        for x in pair_copies(part, s_sem, r_sem):
            x.wait_send()


def per_device(
    n,
    T,
    hidden,
    lengths,
    key_cache,
    value_cache,
    gain_in,
    w_query,
    w_key,
    w_value,
    w_output,
    gain_post,
    w_gate,
    w_up,
    w_down,
):
    S, Dl = hidden.shape
    L = key_cache.shape[1]
    QC, KC = w_query.shape[1], w_key.shape[1]
    O = KC // HD
    PG = QC // KC
    FT = w_gate.shape[1] // HD
    assert n >= O and n % 2 == 0 and FT % O == 0 and PG <= 16
    FO = FT // O
    F0 = FO // 2
    F1 = FO - F0
    QG = PG * HD
    G3 = QG + 2 * HD
    W0, W1 = F0 * HD, F1 * HD
    assert W0 <= QG
    reuse = W1 <= Dl <= G3
    c = dict(n=n, T=T, O=O, S=S, Dl=Dl, L=L, PG=PG, FO=FO, F0=F0, F1=F1, reuse=reuse)
    half = np.arange(HD) % (HD // 2)
    freq = jnp.asarray((rope_base ** (-half * 2.0 / HD)).astype(np.float32)[None, :])
    dma = pltpu.SemaphoreType.DMA
    V = pltpu.VMEM
    anywhere = pl.BlockSpec(memory_space=pl.ANY)
    vmem = pl.BlockSpec(memory_space=pltpu.VMEM)
    packed = pl.pallas_call(
        functools.partial(layer_kernel, c),
        out_shape=jax.ShapeDtypeStruct((S, Dl + 2 * KC), BF),
        in_specs=[anywhere] * 14,
        out_specs=vmem,
        scratch_shapes=[
            pltpu.SMEM(lengths.shape, jnp.int32),
            V((S, Dl), BF),
            V((1, Dl), F32),
            V((1, Dl), F32),
            V((1, HD), F32),
            V((O, Dl, G3), BF),
            V((1, 16, HD) if reuse else (O, W1, Dl), BF),
            V((QC, Dl), BF),
            V((Dl, FT * HD), BF),
            V((Dl, FT * HD), BF),
            V(key_cache.shape, BF),
            V(value_cache.shape, BF),
            V((O, S, G3 + HD), BF),
            V((T, n, S, G3 + HD), BF),
            V((T, S, QG), BF),
            V((T, S, 2 * HD), BF),
            V((T, S, HD), F32),
            V((O, S, QG), BF),
            V((O, S, 2 * HD), BF),
            V((O, S, QG + HD), BF),
            V((T, n, S, QG + HD), BF),
            V((T, S, QG), BF),
            V((O, S, QG), BF),
            V((T, S, Dl), F32),
            V((O, S, 2 * W0 + HD), BF),
            V((O, S, 2 * W1), BF),
            V((T, n, S, 2 * W0 + HD), BF),
            V((T, n, S, 2 * W1), BF),
            V((T, S, W0), BF),
            V((T, S, W1), BF),
            V((O, S, W0), BF),
            V((O, S, W1), BF),
            V((T, S, Dl), F32),
            dma((5,)),
            dma((5,)),
            dma((O, 2, 3)),
            dma((2, O)),
            dma((O,)),
            dma((T, n)),
            dma((T, n)),
            dma((O,)),
            dma((T, n)),
            dma((O,)),
            dma((O,)),
            dma((T, n)),
            dma((T, n)),
            dma((O,)),
            dma((T,)),
            dma((T,)),
            dma((O, 2)),
            dma((T, n, 2)),
            dma((2, T, n)),
            dma((O, 2)),
            dma((T,)),
            dma((T,)),
        ],
        compiler_params=pltpu.CompilerParams(
            collective_id=0, has_side_effects=True, vmem_limit_bytes=67000000
        ),
    )(
        lengths,
        hidden,
        gain_in[None, :],
        gain_post[None, :],
        freq,
        key_cache,
        value_cache,
        w_query,
        w_key,
        w_value,
        w_output,
        w_gate,
        w_up,
        w_down,
    )
    return pl.pallas_call(
        split_kernel,
        out_shape=(
            jax.ShapeDtypeStruct((S, Dl), BF),
            jax.ShapeDtypeStruct((S, KC), BF),
            jax.ShapeDtypeStruct((S, KC), BF),
        ),
        in_specs=[vmem],
        out_specs=(vmem,) * 3,
    )(packed)


def solution(mesh):
    placed = (
        P("groups", "kvseq"),
        P("groups"),
        P("groups", "kvseq", "tensor"),
        P("groups", "kvseq", "tensor"),
        P("kvseq"),
        P("kvseq", "tensor"),
        P("kvseq", "tensor"),
        P("kvseq", "tensor"),
        P("tensor", "kvseq"),
        P("kvseq"),
        P("kvseq", "tensor"),
        P("kvseq", "tensor"),
        P("tensor", "kvseq"),
    )
    return jax.shard_map(
        functools.partial(per_device, mesh.shape["kvseq"], mesh.shape["tensor"]),
        mesh=mesh,
        in_specs=placed,
        out_specs=(P("groups", "kvseq"), P("groups", "tensor"), P("groups", "tensor")),
        check_vma=False,
    )
```

```python
import functools

import jax
import jax.numpy as jnp
import numpy as np
from jax import lax
from jax.experimental import pallas as pl
from jax.experimental.pallas import tpu as pltpu
from jax.sharding import PartitionSpec as P

HD = 128
epsilon = 1e-06
rope_base = 1000000.0
BF = jnp.bfloat16
F32 = jnp.float32
MESH = pl.DeviceIdType.MESH


def mult(x, m):
    return pl.multiple_of(x, m)


def accumulate(n, load, op=jnp.add):
    u = 8 if n % 8 == 0 else 1

    def group(first, acc):
        for j in range(u):
            x = load(first + j)
            acc = x if acc is None else jax.tree.map(op, acc, x)
        return acc

    acc = group(0, None)
    if n == u:
        return acc
    return lax.fori_loop(1, n // u, lambda i, a: group(i * u, a), acc)


def split_kernel(packed, out, new_keys, new_values):
    Dl, KC = out.shape[1], new_keys.shape[1]
    out[...] = packed[:, :Dl]
    new_keys[...] = packed[:, Dl : Dl + KC]
    new_values[...] = packed[:, Dl + KC :]


def layer_kernel(
    c,
    lengths_hbm,
    hidden_hbm,
    gain_in_hbm,
    gain_post_hbm,
    freq_hbm,
    kc_hbm,
    vc_hbm,
    wq_hbm,
    wk_hbm,
    wv_hbm,
    wo_hbm,
    wg_hbm,
    wu_hbm,
    wd_hbm,
    out,
    lengths,
    hidden,
    gain_in,
    gain_post,
    freq,
    wqkv,
    tail,
    wo,
    wg,
    wu,
    kc,
    vc,
    send_a,
    recv_a,
    qg,
    kvg,
    own_scores,
    all_q,
    all_kv,
    send_b,
    recv_b,
    ab,
    all_b,
    part_1,
    send_c0,
    send_c1,
    recv_c0,
    recv_c1,
    ic0,
    ic1,
    all_c0,
    all_c1,
    part_2,
    ssem,
    wsem,
    fsem,
    dsem,
    sa_s,
    sa_r,
    ga_s,
    ga_r,
    gk_s,
    gk_r,
    sb_s,
    sb_r,
    gb_s,
    gb_r,
    t1_s,
    t1_r,
    sc_s,
    sc_r,
    gc_s,
    gc_r,
    t2_s,
    t2_r,
):
    n, T, O = c["n"], c["T"], c["O"]
    S, Dl, L = c["S"], c["Dl"], c["L"]
    PG, FO, F0, F1 = c["PG"], c["FO"], c["F0"], c["F1"]
    QG = PG * HD
    G3 = QG + 2 * HD
    KC = O * HD
    W0, W1 = F0 * HD, F1 * HD
    D = float(Dl * n)
    base = (n - O) // 2
    me = lax.axis_index("kvseq")
    t = lax.axis_index("tensor")
    owner = (me >= base) & (me < base + O) & (t == T - 1)
    o_me = me - base
    half_n = n // 2
    side = me // half_n

    def mine(o):
        return (me == base + o) & (t == T - 1)

    def order(k):
        if O != 4:
            return lax.rem(me + k, O)
        oz = (side + 1 + k // 2) % 2
        oy = (me + 1 + k % 2) % 2
        return oz * 2 + oy

    def near(k):
        return order(O - 1 - k)

    def local(src, dst, sem):
        return pltpu.make_async_copy(src, dst, sem)

    small = [
        local(hidden_hbm, hidden, ssem.at[0]),
        local(gain_in_hbm, gain_in, ssem.at[1]),
        local(lengths_hbm, lengths, ssem.at[2]),
        local(freq_hbm, freq, ssem.at[3]),
        local(gain_post_hbm, gain_post, ssem.at[4]),
    ]
    half = Dl // 2

    def first(k):
        o = order(k)
        return [
            [
                local(
                    src.at[pl.ds(b * half, half), pl.ds(mult(o * width, HD), width)],
                    wqkv.at[k, pl.ds(b * half, half), pl.ds(at, width)],
                    fsem.at[k, b],
                )
                for src, at, width in (
                    (wq_hbm, 0, QG),
                    (wk_hbm, QG, HD),
                    (wv_hbm, QG + HD, HD),
                )
            ]
            for b in range(2)
        ]

    firsts = [first(k) for k in range(O)]

    def first_wait(k, b):
        rows = pl.ds(b * half, half)
        local(wq_hbm.at[rows, pl.ds(0, G3)], wqkv.at[k, rows, :], fsem.at[k, b]).wait()

    kv_copies = [local(kc_hbm, kc, wsem.at[0]), local(vc_hbm, vc, wsem.at[1])]
    later = [
        local(wo_hbm, wo, wsem.at[2]),
        local(wg_hbm, wg, wsem.at[3]),
        local(wu_hbm, wu, wsem.at[4]),
    ]

    def down_0(o):
        return wo.at[pl.ds(mult(o * QG, HD), W0), :]

    def down_1(o):
        return wqkv.at[o, pl.ds(0, W1), pl.ds(0, Dl)] if c["reuse"] else tail.at[o]

    downs_0 = [
        local(wd_hbm.at[pl.ds(o * FO * HD, W0), :], down_0(o), dsem.at[0]) for o in range(O)
    ]
    downs_1 = [
        local(wd_hbm.at[pl.ds((o * FO + F0) * HD, W1), :], down_1(o), dsem.at[1])
        for o in range(O)
    ]
    for x in small:
        x.start()
    for k in range(O):
        for b in range(2):
            for x in firsts[k][b]:
                x.start(priority=1)

    barrier = pltpu.get_barrier_semaphore()
    for dt in range(T):

        def greet(k, _):
            pl.semaphore_signal(
                barrier,
                inc=1,
                device_id={"kvseq": lax.rem(me + k, n), "tensor": lax.rem(t + dt, T)},
                device_id_type=MESH,
            )
            return 0

        lax.fori_loop(0 if dt else 1, n, greet, 0)

    def remote(src, dst, s_sem, r_sem, k, tt):
        return pltpu.make_async_remote_copy(
            src_ref=src, dst_ref=dst, send_sem=s_sem, recv_sem=r_sem,
            device_id={"kvseq": k, "tensor": tt}, device_id_type=MESH,
        )

    def to_owner(src, recv, s_sem, r_sem, o):
        return remote(src, recv, s_sem, r_sem, base + o, T - 1)

    def scatter(src, dst, s_sem, r_sem, o):
        @pl.when(jnp.logical_not(mine(o)))
        def _():
            to_owner(src, dst, s_sem, r_sem, o).start()

        @pl.when(mine(o))
        def _():
            dst[...] = src[...]

    def scatter_wait_send(send, s_sem):
        @pl.when(jnp.logical_not(owner))
        def _():
            remote(send, send, s_sem, s_sem, me, t).wait_send()

        @pl.when(owner)
        def _():
            x = send.at[pl.ds(0, O - 1)]
            remote(x, x, s_sem, s_sem, me, t).wait_send()

    def arrivals(tt):
        return pl.ds(0, n - 1 if tt == T - 1 else n)

    def owner_wait(recv, r_sem, tt):
        x = recv.at[tt, arrivals(tt)]
        remote(x, x, sa_s, r_sem, me, tt).wait_recv()

    def each_target(f):
        def cross(k, _):
            f(k + (1 - side) * (n - 1 - 2 * k))
            return 0

        def same(k, _):
            f(k + side * (n - 1 - 2 * k))
            return 0

        lax.fori_loop(0, half_n, cross, 0)
        lax.fori_loop(0, n - half_n, same, 0)

    def spread(src, dst, s_sem, r_sem, tt, rising=False):
        def one(d):
            def send():
                remote(src, dst, s_sem.at[tt], r_sem, d, tt).start()

            if tt == T - 1:
                pl.when(d != me)(send)
            else:
                send()

        if rising:
            lax.fori_loop(0, n, lambda d, _: (one(d), 0)[1], 0)
        else:
            each_target(one)
        if tt == T - 1:
            dst[...] = src[...]

    def spread_wait_send(like, width, s_sem, tt):
        x = like.at[tt, arrivals(tt), :, pl.ds(0, width)]
        remote(x, x, s_sem.at[tt], s_sem.at[tt], me, tt).wait_send()

    def spread_wait(dst, s_sem, r_sem, o):
        @pl.when(jnp.logical_not(mine(o)))
        def _():
            remote(dst, dst, s_sem.at[0], r_sem, base + o, T - 1).wait_recv()

    def pair_copies(part, s_sem, r_sem):
        return [
            remote(
                part.at[t], part.at[t], s_sem.at[k - 1], r_sem.at[k - 1], me, lax.rem(t + k, T)
            )
            for k in range(1, T)
        ]

    def pair_sum(part, s_sem, r_sem):
        for x in pair_copies(part, s_sem, r_sem):
            x.start()
        for k in range(1, T):
            src = lax.rem(t + T - k, T)
            x = part.at[src]
            remote(x, x, s_sem.at[k - 1], r_sem.at[k - 1], me, src).wait_recv()
        total = part[0]
        for i in range(1, T):
            total = total + part[i]
        return total

    lane = lax.broadcasted_iota(jnp.int32, (S, HD), 1)
    row = lax.broadcasted_iota(jnp.int32, (S, HD), 0)

    def squares_block(x):
        s = jnp.broadcast_to(jnp.sum(x * x, axis=1, keepdims=True), (S, HD))
        high = s.astype(BF).astype(F32)
        return jnp.where(lane < HD // 2, high, s - high).astype(BF)

    def row_scale(block):
        total = jnp.sum(block, axis=1, keepdims=True) * (2.0 / HD)
        return lax.rsqrt(total / D + epsilon)

    small[0].wait()
    small[1].wait()
    stream = hidden[...].astype(F32)
    xg = (stream * gain_in[...]).astype(BF)
    sq = squares_block(stream)

    for k in range(O):
        o = order(k)
        first_wait(k, 0)
        part = jnp.dot(xg[:, :half], wqkv[k, :half, :], preferred_element_type=F32)
        first_wait(k, 1)
        if k == max(O - 2, 0):
            for x in kv_copies:
                x.start(priority=1)
        part = part + jnp.dot(xg[:, half:], wqkv[k, half:, :], preferred_element_type=F32)
        send_a[k, :, :G3] = part.astype(BF)
        send_a[k, :, G3:] = sq
        if k == 0:
            pl.semaphore_wait(barrier, n * T - 1)
        scatter(send_a.at[k], recv_a.at[t, me], sa_s, sa_r.at[t], o)
    for x in later + downs_1:
        x.start(priority=1)

    small[2].wait()
    small[3].wait()
    position = jnp.zeros((S, HD), F32)
    for s in range(S):
        position = jnp.where(row == s, lengths[s].astype(F32), position)
    angle = position * freq[...]
    cosine = jnp.cos(angle)
    sine = jnp.sin(angle)
    sine = jnp.where(lane < HD // 2, -sine, sine)
    factor = float(HD) ** (-0.5)

    @pl.when(owner)
    def _():
        for tt in reversed(range(T)):
            owner_wait(recv_a, sa_r.at[tt], tt)
            total = accumulate(n, lambda k: recv_a[tt, k].astype(F32))
            scale = row_scale(total[:, G3:])
            for j in range(PG + 1):
                v = total[:, j * HD : (j + 1) * HD] * scale
                v = (v * cosine + pltpu.roll(v, HD // 2, 1) * sine).astype(BF)
                if j < PG:
                    qg[tt, :, j * HD : (j + 1) * HD] = v
                else:
                    kvg[tt, :, :HD] = v
            kvg[tt, :, HD:] = (total[:, QG + HD : G3] * scale).astype(BF)
            spread(qg.at[tt], all_q.at[o_me], ga_s, ga_r.at[o_me], tt)
        for tt in range(T):
            spread(kvg.at[tt], all_kv.at[o_me], gk_s, gk_r, tt)
        for tt in range(T):
            key = kvg[tt, :, :HD].astype(F32)
            block = jnp.zeros((S, HD), F32)
            for j in range(PG):
                q = qg[tt, :, j * HD : (j + 1) * HD].astype(F32)
                block = jnp.where(
                    lane == j, jnp.sum(q * key, axis=1, keepdims=True) * factor, block
                )
            own_scores[tt] = block

    R = PG * S
    brow = lax.broadcasted_iota(jnp.int32, (R, L), 0) % S
    orow = lax.broadcasted_iota(jnp.int32, (R, HD), 0) % S
    limit = jnp.zeros((R, L), jnp.int32)
    for s in range(S):
        limit = jnp.where(brow == s, lengths[s], limit)
    place = lax.broadcasted_iota(jnp.int32, (R, L), 1) + me * L
    valid = place < limit
    for x in kv_copies:
        x.wait()
    group = lane % 16
    third = (lane % (HD // 2)) // 16

    def attend_one(g):
        q = jnp.concatenate(
            [all_q[g, :, j * HD : (j + 1) * HD].astype(F32) for j in range(PG)], axis=0
        ).astype(BF)
        cols = pl.ds(mult(g * HD, HD), HD)
        scores = jnp.zeros((R, L), F32)
        for s in range(S):
            x = lax.dot_general(
                q, kc[s, :, cols], (((1,), (1,)), ((), ())), preferred_element_type=F32
            )
            scores = jnp.where(brow == s, x, scores)
        scores = jnp.where(valid, scores * factor, -1e30)
        top = jnp.max(scores, axis=1, keepdims=True)
        w = jnp.where(valid, jnp.exp(scores - top), 0.0)
        total = jnp.sum(w, axis=1, keepdims=True)
        w = w.astype(BF)
        mixed = jnp.zeros((R, HD), F32)
        for s in range(S):
            x = jnp.dot(w, vc[s, :, cols], preferred_element_type=F32)
            mixed = jnp.where(orow == s, x, mixed)
        ml = jnp.zeros((S, HD), F32)
        for j in range(PG):
            rows = slice(j * S, (j + 1) * S)
            send_b[g, :, j * HD : (j + 1) * HD] = mixed[rows].astype(BF)
            ml = jnp.where(group == j, jnp.where(lane < HD // 2, top[rows], total[rows]), ml)
        high = ml.astype(BF).astype(F32)
        rest = ml - high
        middle = rest.astype(BF).astype(F32)
        low = rest - middle
        parts = jnp.where(third == 0, high, jnp.where(third == 1, middle, low))
        send_b[g, :, QG:] = parts.astype(BF)

    step = 1

    def attend(i, _):
        blocks = [near(i * step + j) for j in range(step)]
        for g in blocks:
            spread_wait(all_q.at[g], ga_s, ga_r.at[g], g)
        for g in blocks:
            attend_one(g)
        for g in blocks:
            scatter(send_b.at[g], recv_b.at[t, me], sb_s, sb_r.at[t], g)
        return 0

    lax.fori_loop(0, O // step, attend, 0)

    @pl.when(owner)
    def _():
        for tt in reversed(range(T)):
            owner_wait(recv_b, sb_r.at[tt], tt)

            def stats(k):
                x = recv_b[tt, k, :, QG:].astype(F32)
                return x + pltpu.roll(x, HD - 16, 1) + pltpu.roll(x, HD - 32, 1)

            top = accumulate(n, stats, jnp.maximum)
            total = accumulate(
                n, lambda k: pltpu.roll(stats(k), HD // 2, 1) * jnp.exp(stats(k) - top)
            )
            own = own_scores[tt]
            best = jnp.maximum(top, own)
            old_scale = jnp.exp(top - best)
            own_weight = jnp.exp(own - best)
            bottom = total * old_scale + own_weight
            old_scale = old_scale / bottom
            own_weight = own_weight / bottom

            def weighted(k):
                scale = jnp.exp(stats(k) - top) * old_scale
                return tuple(
                    recv_b[tt, k, :, j * HD : (j + 1) * HD].astype(F32) * scale[:, j : j + 1]
                    for j in range(PG)
                )

            mixed = accumulate(n, weighted)
            val = kvg[tt, :, HD:].astype(F32)
            for j in range(PG):
                res = mixed[j] + own_weight[:, j : j + 1] * val
                ab[tt, :, j * HD : (j + 1) * HD] = res.astype(BF)
            spread(ab.at[tt], all_b.at[o_me], gb_s, gb_r.at[o_me], tt)

    later[0].wait()

    def output_block(i, acc):
        g = near(i)
        spread_wait(all_b.at[g], gb_s, gb_r.at[g], g)
        w = wo[pl.ds(mult(g * QG, HD), QG), :]
        return acc + jnp.dot(all_b[g], w, preferred_element_type=F32)

    part_1[t] = lax.fori_loop(0, O, output_block, jnp.zeros((S, Dl), F32))
    for x in downs_0:
        x.start(priority=1)
    small[4].wait()
    residual = hidden[...].astype(F32) + pair_sum(part_1, t1_s, t1_r)
    sq_post = squares_block(residual)
    rg = (residual * gain_post[...]).astype(BF)
    later[1].wait()
    later[2].wait()

    def widen(k, _):
        o = order(k)
        for send, recv, i, at, W in (
            (send_c0, recv_c0, 0, 0, W0),
            (send_c1, recv_c1, 1, F0, W1),
        ):
            begin = (o * FO + at) * HD
            for b, w in enumerate((wg, wu)):
                for j in range(0, W, 256):
                    step = min(256, W - j)
                    x = jnp.dot(
                        rg, w[:, pl.ds(mult(begin + j, HD), step)], preferred_element_type=F32
                    )
                    send[o, :, b * W + j : b * W + j + step] = x.astype(BF)
            if i == 0:
                send[o, :, 2 * W :] = sq_post
            scatter(send.at[o], recv.at[t, me], sc_s.at[i], sc_r.at[t, i], o)
        return 0

    lax.fori_loop(0, O, widen, 0)

    @pl.when(jnp.logical_not(owner))
    def _():
        remote(all_kv, all_kv, gk_s.at[0], gk_r, me, t).wait_recv()

    @pl.when(owner)
    def _():
        x = all_kv.at[pl.ds(0, O - 1)]
        remote(x, x, gk_s.at[0], gk_r, me, t).wait_recv()

    for g in range(O):
        out[:, Dl + g * HD : Dl + (g + 1) * HD] = all_kv[g, :, :HD]
        out[:, Dl + KC + g * HD : Dl + KC + (g + 1) * HD] = all_kv[g, :, HD:]

    @pl.when(owner)
    def _():
        scales = [None] * T
        for i, recv, ic, all_c, W in ((0, recv_c0, ic0, all_c0, W0), (1, recv_c1, ic1, all_c1, W1)):
            for tt in reversed(range(T)):
                owner_wait(recv, sc_r.at[tt, i], tt)
                if i == 0:
                    scales[tt] = row_scale(
                        accumulate(n, lambda k: recv[tt, k, :, 2 * W :].astype(F32))
                    )
                for j in range(0, W, HD):
                    gate = accumulate(n, lambda k: recv[tt, k, :, j : j + HD].astype(F32))
                    up = accumulate(n, lambda k: recv[tt, k, :, W + j : W + j + HD].astype(F32))
                    gate = gate * scales[tt]
                    up = up * scales[tt]
                    ic[tt, :, j : j + HD] = (gate * jax.nn.sigmoid(gate) * up).astype(BF)
                spread(ic.at[tt], all_c.at[o_me], gc_s.at[i], gc_r.at[o_me, i], tt, rising=True)

    for i, W in ((0, W0), (1, W1)):
        rows = pl.ds(0, O * W)
        local(wd_hbm.at[rows, :], wo.at[rows, :], dsem.at[i]).wait()

    def down_block(k, acc):
        o = near(k)
        spread_wait(all_c0.at[o], gc_s.at[0], gc_r.at[o, 0], o)
        acc = acc + jnp.dot(all_c0[o], down_0(o)[...], preferred_element_type=F32)
        spread_wait(all_c1.at[o], gc_s.at[1], gc_r.at[o, 1], o)
        return acc + jnp.dot(all_c1[o], down_1(o)[...], preferred_element_type=F32)

    part_2[t] = lax.fori_loop(0, O, down_block, jnp.zeros((S, Dl), F32))
    out[:, :Dl] = (residual + pair_sum(part_2, t2_s, t2_r)).astype(BF)

    for send, s_sem in (
        (send_a, sa_s),
        (send_b, sb_s),
        (send_c0, sc_s.at[0]),
        (send_c1, sc_s.at[1]),
    ):
        scatter_wait_send(send, s_sem)

    @pl.when(owner)
    def _():
        for tt in range(T):
            spread_wait_send(recv_b, QG, ga_s, tt)
            spread_wait_send(recv_b, 2 * HD, gk_s, tt)
            spread_wait_send(recv_b, QG, gb_s, tt)
            spread_wait_send(recv_c0, W0, gc_s.at[0], tt)
            spread_wait_send(recv_c1, W1, gc_s.at[1], tt)

    for part, s_sem, r_sem in ((part_1, t1_s, t1_r), (part_2, t2_s, t2_r)):
        for x in pair_copies(part, s_sem, r_sem):
            x.wait_send()


def per_device(
    n,
    T,
    hidden,
    lengths,
    key_cache,
    value_cache,
    gain_in,
    w_query,
    w_key,
    w_value,
    w_output,
    gain_post,
    w_gate,
    w_up,
    w_down,
):
    S, Dl = hidden.shape
    L = key_cache.shape[1]
    QC, KC = w_query.shape[1], w_key.shape[1]
    O = KC // HD
    PG = QC // KC
    FT = w_gate.shape[1] // HD
    assert n >= O and n % 2 == 0 and FT % O == 0 and PG <= 16
    FO = FT // O
    F0 = FO // 2
    F1 = FO - F0
    QG = PG * HD
    G3 = QG + 2 * HD
    W0, W1 = F0 * HD, F1 * HD
    assert W1 <= QG
    reuse = W1 <= Dl <= G3
    c = dict(n=n, T=T, O=O, S=S, Dl=Dl, L=L, PG=PG, FO=FO, F0=F0, F1=F1, reuse=reuse)
    half = np.arange(HD) % (HD // 2)
    freq = jnp.asarray((rope_base ** (-half * 2.0 / HD)).astype(np.float32)[None, :])
    dma = pltpu.SemaphoreType.DMA
    V = pltpu.VMEM
    anywhere = pl.BlockSpec(memory_space=pl.ANY)
    vmem = pl.BlockSpec(memory_space=pltpu.VMEM)
    packed = pl.pallas_call(
        functools.partial(layer_kernel, c),
        out_shape=pltpu.VMEM((S, Dl + 2 * KC), BF),
        in_specs=[anywhere] * 14,
        out_specs=vmem,
        scratch_shapes=[
            pltpu.SMEM(lengths.shape, jnp.int32),
            V((S, Dl), BF),
            V((1, Dl), F32),
            V((1, Dl), F32),
            V((1, HD), F32),
            V((O, Dl, G3), BF),
            V((1, 16, HD) if reuse else (O, W1, Dl), BF),
            V((QC, Dl), BF),
            V((Dl, FT * HD), BF),
            V((Dl, FT * HD), BF),
            V(key_cache.shape, BF),
            V(value_cache.shape, BF),
            V((O, S, G3 + HD), BF),
            V((T, n, S, G3 + HD), BF),
            V((T, S, QG), BF),
            V((T, S, 2 * HD), BF),
            V((T, S, HD), F32),
            V((O, S, QG), BF),
            V((O, S, 2 * HD), BF),
            V((O, S, QG + HD), BF),
            V((T, n, S, QG + HD), BF),
            V((T, S, QG), BF),
            V((O, S, QG), BF),
            V((T, S, Dl), F32),
            V((O, S, 2 * W0 + HD), BF),
            V((O, S, 2 * W1), BF),
            V((T, n, S, 2 * W0 + HD), BF),
            V((T, n, S, 2 * W1), BF),
            V((T, S, W0), BF),
            V((T, S, W1), BF),
            V((O, S, W0), BF),
            V((O, S, W1), BF),
            V((T, S, Dl), F32),
            dma((5,)),
            dma((5,)),
            dma((O, 2)),
            dma((2,)),
            dma,
            dma((T,)),
            dma((T,)),
            dma((O,)),
            dma((T,)),
            dma,
            dma,
            dma((T,)),
            dma((T,)),
            dma((O,)),
            dma((T - 1,)),
            dma((T - 1,)),
            dma((2,)),
            dma((T, 2)),
            dma((2, T)),
            dma((O, 2)),
            dma((T - 1,)),
            dma((T - 1,)),
        ],
        compiler_params=pltpu.CompilerParams(
            collective_id=0, has_side_effects=True, vmem_limit_bytes=67000000
        ),
    )(
        lengths,
        hidden,
        gain_in[None, :],
        gain_post[None, :],
        freq,
        key_cache,
        value_cache,
        w_query,
        w_key,
        w_value,
        w_output,
        w_gate,
        w_up,
        w_down,
    )
    return pl.pallas_call(
        split_kernel,
        out_shape=(
            jax.ShapeDtypeStruct((S, Dl), BF),
            jax.ShapeDtypeStruct((S, KC), BF),
            jax.ShapeDtypeStruct((S, KC), BF),
        ),
        in_specs=[vmem],
        out_specs=(vmem,) * 3,
    )(pltpu.with_memory_space_constraint(packed, pltpu.VMEM))


def solution(mesh):
    placed = (
        P("groups", "kvseq"),
        P("groups"),
        P("groups", "kvseq", "tensor"),
        P("groups", "kvseq", "tensor"),
        P("kvseq"),
        P("kvseq", "tensor"),
        P("kvseq", "tensor"),
        P("kvseq", "tensor"),
        P("tensor", "kvseq"),
        P("kvseq"),
        P("kvseq", "tensor"),
        P("kvseq", "tensor"),
        P("tensor", "kvseq"),
    )
    return jax.shard_map(
        functools.partial(per_device, mesh.shape["kvseq"], mesh.shape["tensor"]),
        mesh=mesh,
        in_specs=placed,
        out_specs=(P("groups", "kvseq"), P("groups", "tensor"), P("groups", "tensor")),
        check_vma=False,
    )
```

```python
import functools

import jax
import jax.numpy as jnp
import numpy as np
from jax import lax
from jax.experimental import pallas as pl
from jax.experimental.pallas import tpu as pltpu
from jax.sharding import PartitionSpec as P

HD = 128
epsilon = 1e-06
ATTEND_ORDER = (0, 3, 2, 1)
rope_base = 1000000.0
BF = jnp.bfloat16
F32 = jnp.float32
MESH = pl.DeviceIdType.MESH


def mult(x, m):
    return pl.multiple_of(x, m)


def accumulate(n, load, op=jnp.add):
    u = 8 if n % 8 == 0 else 1

    def group(first, acc):
        for j in range(u):
            x = load(first + j)
            acc = x if acc is None else jax.tree.map(op, acc, x)
        return acc

    acc = group(0, None)
    if n == u:
        return acc
    return lax.fori_loop(1, n // u, lambda i, a: group(i * u, a), acc)


def split_kernel(packed, out, new_keys, new_values):
    Dl, KC = out.shape[1], new_keys.shape[1]
    out[...] = packed[:, :Dl]
    new_keys[...] = packed[:, Dl : Dl + KC]
    new_values[...] = packed[:, Dl + KC :]


def layer_kernel(
    c,
    lengths_hbm,
    hidden_hbm,
    gain_in_hbm,
    gain_post_hbm,
    freq_hbm,
    kc_hbm,
    vc_hbm,
    wq_hbm,
    wk_hbm,
    wv_hbm,
    wo_hbm,
    wg_hbm,
    wu_hbm,
    wd_hbm,
    out,
    lengths,
    hidden,
    gain_in,
    gain_post,
    freq,
    wqkv,
    tail,
    wo,
    wg,
    wu,
    kc,
    vc,
    send_a,
    recv_a,
    qg,
    kvg,
    own_scores,
    all_q,
    all_kv,
    send_b,
    recv_b,
    ab,
    all_b,
    part_1,
    send_c0,
    send_c1,
    recv_c0,
    recv_c1,
    ic0,
    ic1,
    all_c0,
    all_c1,
    part_2,
    ssem,
    wsem,
    fsem,
    dsem,
    sa_s,
    sa_r,
    ga_s,
    ga_r,
    gk_s,
    gk_r,
    sb_s,
    sb_r,
    gb_s,
    gb_r,
    t1_s,
    t1_r,
    sc_s,
    sc_r,
    gc_s,
    gc_r,
    t2_s,
    t2_r,
):
    n, T, O = c["n"], c["T"], c["O"]
    S, Dl, L = c["S"], c["Dl"], c["L"]
    PG, FO, F0, F1 = c["PG"], c["FO"], c["F0"], c["F1"]
    QG = PG * HD
    G3 = QG + 2 * HD
    KC = O * HD
    W0, W1 = F0 * HD, F1 * HD
    D = float(Dl * n)
    base = (n - O) // 2
    me = lax.axis_index("kvseq")
    t = lax.axis_index("tensor")
    owner = (me >= base) & (me < base + O) & (t == T - 1)
    o_me = me - base
    half_n = n // 2
    side = me // half_n

    def mine(o):
        return (me == base + o) & (t == T - 1)

    def order(k):
        if O != 4:
            return lax.rem(me + k, O)
        oz = (side + 1 + k // 2) % 2
        oy = (me + 1 + k % 2) % 2
        return oz * 2 + oy

    def near(k):
        return order(O - 1 - k)

    def local(src, dst, sem):
        return pltpu.make_async_copy(src, dst, sem)

    small = [
        local(hidden_hbm, hidden, ssem.at[0]),
        local(gain_in_hbm, gain_in, ssem.at[1]),
        local(lengths_hbm, lengths, ssem.at[2]),
        local(freq_hbm, freq, ssem.at[3]),
        local(gain_post_hbm, gain_post, ssem.at[4]),
    ]
    half = Dl // 2

    def first(k):
        o = order(k)
        return [
            [
                local(
                    src.at[pl.ds(b * half, half), pl.ds(mult(o * width, HD), width)],
                    wqkv.at[k, pl.ds(b * half, half), pl.ds(at, width)],
                    fsem.at[k, b],
                )
                for src, at, width in (
                    (wq_hbm, 0, QG),
                    (wk_hbm, QG, HD),
                    (wv_hbm, QG + HD, HD),
                )
            ]
            for b in range(2)
        ]

    firsts = [first(k) for k in range(O)]

    def first_wait(k, b):
        rows = pl.ds(b * half, half)
        local(wq_hbm.at[rows, pl.ds(0, G3)], wqkv.at[k, rows, :], fsem.at[k, b]).wait()

    kv_copies = [local(kc_hbm, kc, wsem.at[0]), local(vc_hbm, vc, wsem.at[1])]
    later = [
        local(wo_hbm, wo, wsem.at[2]),
        local(wg_hbm, wg, wsem.at[3]),
        local(wu_hbm, wu, wsem.at[4]),
    ]

    def down_0(o):
        return wo.at[pl.ds(mult(o * QG, HD), W0), :]

    def down_1(o):
        return wqkv.at[o, pl.ds(0, W1), pl.ds(0, Dl)] if c["reuse"] else tail.at[o]

    downs_0 = [
        local(wd_hbm.at[pl.ds(o * FO * HD, W0), :], down_0(o), dsem.at[0]) for o in range(O)
    ]
    downs_1 = [
        local(wd_hbm.at[pl.ds((o * FO + F0) * HD, W1), :], down_1(o), dsem.at[1])
        for o in range(O)
    ]
    for x in small:
        x.start()
    for k in range(O):
        for b in range(2):
            for x in firsts[k][b]:
                x.start(priority=1)

    barrier = pltpu.get_barrier_semaphore()
    for dt in range(T):

        def greet(k, _):
            pl.semaphore_signal(
                barrier,
                inc=1,
                device_id={"kvseq": lax.rem(me + k, n), "tensor": lax.rem(t + dt, T)},
                device_id_type=MESH,
            )
            return 0

        lax.fori_loop(0 if dt else 1, n, greet, 0)

    def remote(src, dst, s_sem, r_sem, k, tt):
        return pltpu.make_async_remote_copy(
            src_ref=src, dst_ref=dst, send_sem=s_sem, recv_sem=r_sem,
            device_id={"kvseq": k, "tensor": tt}, device_id_type=MESH,
        )

    def to_owner(src, recv, s_sem, r_sem, o):
        return remote(src, recv, s_sem, r_sem, base + o, T - 1)

    def scatter(src, dst, s_sem, r_sem, o):
        @pl.when(jnp.logical_not(mine(o)))
        def _():
            to_owner(src, dst, s_sem, r_sem, o).start()

        @pl.when(mine(o))
        def _():
            dst[...] = src[...]

    def scatter_wait_send(send, s_sem):
        @pl.when(jnp.logical_not(owner))
        def _():
            remote(send, send, s_sem, s_sem, me, t).wait_send()

        @pl.when(owner)
        def _():
            x = send.at[pl.ds(0, O - 1)]
            remote(x, x, s_sem, s_sem, me, t).wait_send()

    def arrivals(tt):
        return pl.ds(0, n - 1 if tt == T - 1 else n)

    def owner_wait(recv, r_sem, tt):
        x = recv.at[tt, arrivals(tt)]
        remote(x, x, sa_s, r_sem, me, tt).wait_recv()

    def each_target(f):
        def cross(k, _):
            f(k + (1 - side) * (n - 1 - 2 * k))
            return 0

        def same(k, _):
            f(k + side * (n - 1 - 2 * k))
            return 0

        lax.fori_loop(0, half_n, cross, 0)
        lax.fori_loop(0, n - half_n, same, 0)

    def spread(src, dst, s_sem, r_sem, tt, rising=False):
        def one(d):
            def send():
                remote(src, dst, s_sem.at[tt], r_sem, d, tt).start()

            if tt == T - 1:
                pl.when(d != me)(send)
            else:
                send()

        if rising:
            lax.fori_loop(0, n, lambda d, _: (one(d), 0)[1], 0)
        else:
            each_target(one)
        if tt == T - 1:
            dst[...] = src[...]

    def spread_wait_send(like, width, s_sem, tt):
        x = like.at[tt, arrivals(tt), :, pl.ds(0, width)]
        remote(x, x, s_sem.at[tt], s_sem.at[tt], me, tt).wait_send()

    def spread_wait(dst, s_sem, r_sem, o):
        @pl.when(jnp.logical_not(mine(o)))
        def _():
            remote(dst, dst, s_sem.at[0], r_sem, base + o, T - 1).wait_recv()

    def pair_copies(part, s_sem, r_sem):
        return [
            remote(
                part.at[t], part.at[t], s_sem.at[k - 1], r_sem.at[k - 1], me, lax.rem(t + k, T)
            )
            for k in range(1, T)
        ]

    def pair_sum(part, s_sem, r_sem):
        for x in pair_copies(part, s_sem, r_sem):
            x.start()
        for k in range(1, T):
            src = lax.rem(t + T - k, T)
            x = part.at[src]
            remote(x, x, s_sem.at[k - 1], r_sem.at[k - 1], me, src).wait_recv()
        total = part[0]
        for i in range(1, T):
            total = total + part[i]
        return total

    lane = lax.broadcasted_iota(jnp.int32, (S, HD), 1)
    row = lax.broadcasted_iota(jnp.int32, (S, HD), 0)

    def squares_block(x):
        s = jnp.broadcast_to(jnp.sum(x * x, axis=1, keepdims=True), (S, HD))
        high = s.astype(BF).astype(F32)
        return jnp.where(lane < HD // 2, high, s - high).astype(BF)

    def row_scale(block):
        total = jnp.sum(block, axis=1, keepdims=True) * (2.0 / HD)
        return lax.rsqrt(total / D + epsilon)

    small[0].wait()
    small[1].wait()
    stream = hidden[...].astype(F32)
    xg = (stream * gain_in[...]).astype(BF)
    sq = squares_block(stream)

    for k in range(O):
        o = order(k)
        first_wait(k, 0)
        part = jnp.dot(xg[:, :half], wqkv[k, :half, :], preferred_element_type=F32)
        first_wait(k, 1)
        if k == max(O - 2, 0):
            for x in kv_copies:
                x.start(priority=1)
        part = part + jnp.dot(xg[:, half:], wqkv[k, half:, :], preferred_element_type=F32)
        send_a[k, :, :G3] = part.astype(BF)
        send_a[k, :, G3:] = sq
        if k == 0:
            pl.semaphore_wait(barrier, n * T - 1)
        scatter(send_a.at[k], recv_a.at[t, me], sa_s, sa_r.at[t], o)
    for x in later + downs_1:
        x.start(priority=1)

    small[2].wait()
    small[3].wait()
    position = jnp.zeros((S, HD), F32)
    for s in range(S):
        position = jnp.where(row == s, lengths[s].astype(F32), position)
    angle = position * freq[...]
    cosine = jnp.cos(angle)
    sine = jnp.sin(angle)
    sine = jnp.where(lane < HD // 2, -sine, sine)
    factor = float(HD) ** (-0.5)

    @pl.when(owner)
    def _():
        scale = None
        for tt in reversed(range(T)):
            owner_wait(recv_a, sa_r.at[tt], tt)
            total = accumulate(n, lambda k: recv_a[tt, k].astype(F32))
            if scale is None:
                scale = row_scale(total[:, G3:])
            for j in range(PG + 1):
                v = total[:, j * HD : (j + 1) * HD]
                v = ((v * cosine + pltpu.roll(v, HD // 2, 1) * sine) * scale).astype(BF)
                if j < PG:
                    qg[tt, :, j * HD : (j + 1) * HD] = v
                else:
                    kvg[tt, :, :HD] = v
            kvg[tt, :, HD:] = (total[:, QG + HD : G3] * scale).astype(BF)
            spread(qg.at[tt], all_q.at[o_me], ga_s, ga_r.at[o_me], tt)
        for tt in range(T):
            spread(kvg.at[tt], all_kv.at[o_me], gk_s, gk_r, tt)
        for tt in range(T):
            key = kvg[tt, :, :HD].astype(F32)
            block = jnp.zeros((S, HD), F32)
            for j in range(PG):
                q = qg[tt, :, j * HD : (j + 1) * HD].astype(F32)
                block = jnp.where(
                    lane == j, jnp.sum(q * key, axis=1, keepdims=True) * factor, block
                )
            own_scores[tt] = block

    R = PG * S
    brow = lax.broadcasted_iota(jnp.int32, (R, L), 0) % S
    orow = lax.broadcasted_iota(jnp.int32, (R, HD), 0) % S
    limit = jnp.zeros((R, L), jnp.int32)
    for s in range(S):
        limit = jnp.where(brow == s, lengths[s], limit)
    place = lax.broadcasted_iota(jnp.int32, (R, L), 1) + me * L
    valid = place < limit
    for x in kv_copies:
        x.wait()
    group = lane % 16
    third = (lane % (HD // 2)) // 16

    def attend_one(g):
        q = jnp.concatenate(
            [all_q[g, :, j * HD : (j + 1) * HD].astype(F32) for j in range(PG)], axis=0
        ).astype(BF)
        cols = pl.ds(mult(g * HD, HD), HD)
        scores = jnp.zeros((R, L), F32)
        for s in range(S):
            x = lax.dot_general(
                q, kc[s, :, cols], (((1,), (1,)), ((), ())), preferred_element_type=F32
            )
            scores = jnp.where(brow == s, x, scores)
        scores = jnp.where(valid, scores * factor, -1e30)
        top = jnp.max(scores, axis=1, keepdims=True)
        w = jnp.where(valid, jnp.exp(scores - top), 0.0)
        total = jnp.sum(w, axis=1, keepdims=True)
        w = w.astype(BF)
        mixed = jnp.zeros((R, HD), F32)
        for s in range(S):
            x = jnp.dot(w, vc[s, :, cols], preferred_element_type=F32)
            mixed = jnp.where(orow == s, x, mixed)
        ml = jnp.zeros((S, HD), F32)
        for j in range(PG):
            rows = slice(j * S, (j + 1) * S)
            send_b[g, :, j * HD : (j + 1) * HD] = mixed[rows].astype(BF)
            ml = jnp.where(group == j, jnp.where(lane < HD // 2, top[rows], total[rows]), ml)
        high = ml.astype(BF).astype(F32)
        rest = ml - high
        middle = rest.astype(BF).astype(F32)
        low = rest - middle
        parts = jnp.where(third == 0, high, jnp.where(third == 1, middle, low))
        send_b[g, :, QG:] = parts.astype(BF)

    def attend(i, _):
        k = i
        if O == len(ATTEND_ORDER):
            for j, v in enumerate(ATTEND_ORDER):
                k = jnp.where(i == j, v, k)
        g = near(k)
        spread_wait(all_q.at[g], ga_s, ga_r.at[g], g)
        attend_one(g)
        scatter(send_b.at[g], recv_b.at[t, me], sb_s, sb_r.at[t], g)
        return 0

    lax.fori_loop(0, O, attend, 0)

    @pl.when(owner)
    def _():
        for tt in reversed(range(T)):
            owner_wait(recv_b, sb_r.at[tt], tt)

            def stats(k):
                x = recv_b[tt, k, :, QG:].astype(F32)
                return x + pltpu.roll(x, HD - 16, 1) + pltpu.roll(x, HD - 32, 1)

            if n <= 8:
                known = [stats(k) for k in range(n)]
                stats = known.__getitem__
            top = accumulate(n, stats, jnp.maximum)
            total = accumulate(
                n, lambda k: pltpu.roll(stats(k), HD // 2, 1) * jnp.exp(stats(k) - top)
            )
            own = own_scores[tt]
            best = jnp.maximum(top, own)
            old_scale = jnp.exp(top - best)
            own_weight = jnp.exp(own - best)
            bottom = total * old_scale + own_weight
            old_scale = old_scale / bottom
            own_weight = own_weight / bottom

            def weighted(k):
                scale = jnp.exp(stats(k) - top) * old_scale
                return tuple(
                    recv_b[tt, k, :, j * HD : (j + 1) * HD].astype(F32) * scale[:, j : j + 1]
                    for j in range(PG)
                )

            mixed = accumulate(n, weighted)
            val = kvg[tt, :, HD:].astype(F32)
            for j in range(PG):
                res = mixed[j] + own_weight[:, j : j + 1] * val
                ab[tt, :, j * HD : (j + 1) * HD] = res.astype(BF)
            spread(ab.at[tt], all_b.at[o_me], gb_s, gb_r.at[o_me], tt)

    later[0].wait()

    def output_block(i, acc):
        g = near(i)
        spread_wait(all_b.at[g], gb_s, gb_r.at[g], g)
        w = wo[pl.ds(mult(g * QG, HD), QG), :]
        return acc + jnp.dot(all_b[g], w, preferred_element_type=F32)

    part_1[t] = lax.fori_loop(0, O, output_block, jnp.zeros((S, Dl), F32))
    for x in downs_0:
        x.start(priority=1)
    small[4].wait()
    residual = hidden[...].astype(F32) + pair_sum(part_1, t1_s, t1_r)
    sq_post = squares_block(residual)
    rg = (residual * gain_post[...]).astype(BF)
    later[1].wait()
    later[2].wait()

    def widen(k, _):
        o = order(k)
        for send, recv, i, at, W in (
            (send_c0, recv_c0, 0, 0, W0),
            (send_c1, recv_c1, 1, F0, W1),
        ):
            begin = (o * FO + at) * HD
            for b, w in enumerate((wg, wu)):
                for j in range(0, W, 256):
                    step = min(256, W - j)
                    x = jnp.dot(
                        rg, w[:, pl.ds(mult(begin + j, HD), step)], preferred_element_type=F32
                    )
                    send[o, :, b * W + j : b * W + j + step] = x.astype(BF)
            if i == 0:
                send[o, :, 2 * W :] = sq_post
            scatter(send.at[o], recv.at[t, me], sc_s.at[i], sc_r.at[t, i], o)
        return 0

    lax.fori_loop(0, O, widen, 0)

    @pl.when(jnp.logical_not(owner))
    def _():
        remote(all_kv, all_kv, gk_s.at[0], gk_r, me, t).wait_recv()

    @pl.when(owner)
    def _():
        x = all_kv.at[pl.ds(0, O - 1)]
        remote(x, x, gk_s.at[0], gk_r, me, t).wait_recv()

    for g in range(O):
        out[:, Dl + g * HD : Dl + (g + 1) * HD] = all_kv[g, :, :HD]
        out[:, Dl + KC + g * HD : Dl + KC + (g + 1) * HD] = all_kv[g, :, HD:]

    @pl.when(owner)
    def _():
        scales = [None] * T
        for i, recv, ic, all_c, W in ((0, recv_c0, ic0, all_c0, W0), (1, recv_c1, ic1, all_c1, W1)):
            for tt in reversed(range(T)):
                owner_wait(recv, sc_r.at[tt, i], tt)
                if i == 0:
                    scales[tt] = row_scale(
                        accumulate(n, lambda k: recv[tt, k, :, 2 * W :].astype(F32))
                    )
                for j in range(0, W, HD):
                    gate = accumulate(n, lambda k: recv[tt, k, :, j : j + HD].astype(F32))
                    up = accumulate(n, lambda k: recv[tt, k, :, W + j : W + j + HD].astype(F32))
                    gate = gate * scales[tt]
                    up = up * scales[tt]
                    ic[tt, :, j : j + HD] = (gate * jax.nn.sigmoid(gate) * up).astype(BF)
                spread(ic.at[tt], all_c.at[o_me], gc_s.at[i], gc_r.at[o_me, i], tt, rising=True)

    for i, W in ((0, W0), (1, W1)):
        rows = pl.ds(0, O * W)
        local(wd_hbm.at[rows, :], wo.at[rows, :], dsem.at[i]).wait()

    def down_block(k, acc):
        o = near(k)
        spread_wait(all_c0.at[o], gc_s.at[0], gc_r.at[o, 0], o)
        acc = acc + jnp.dot(all_c0[o], down_0(o)[...], preferred_element_type=F32)
        spread_wait(all_c1.at[o], gc_s.at[1], gc_r.at[o, 1], o)
        return acc + jnp.dot(all_c1[o], down_1(o)[...], preferred_element_type=F32)

    part_2[t] = lax.fori_loop(0, O, down_block, jnp.zeros((S, Dl), F32))
    out[:, :Dl] = (residual + pair_sum(part_2, t2_s, t2_r)).astype(BF)

    for send, s_sem in (
        (send_a, sa_s),
        (send_b, sb_s),
        (send_c0, sc_s.at[0]),
        (send_c1, sc_s.at[1]),
    ):
        scatter_wait_send(send, s_sem)

    @pl.when(owner)
    def _():
        for tt in range(T):
            spread_wait_send(recv_b, QG, ga_s, tt)
            spread_wait_send(recv_b, 2 * HD, gk_s, tt)
            spread_wait_send(recv_b, QG, gb_s, tt)
            spread_wait_send(recv_c0, W0, gc_s.at[0], tt)
            spread_wait_send(recv_c1, W1, gc_s.at[1], tt)

    for part, s_sem, r_sem in ((part_1, t1_s, t1_r), (part_2, t2_s, t2_r)):
        for x in pair_copies(part, s_sem, r_sem):
            x.wait_send()


def per_device(
    n,
    T,
    hidden,
    lengths,
    key_cache,
    value_cache,
    gain_in,
    w_query,
    w_key,
    w_value,
    w_output,
    gain_post,
    w_gate,
    w_up,
    w_down,
):
    S, Dl = hidden.shape
    L = key_cache.shape[1]
    QC, KC = w_query.shape[1], w_key.shape[1]
    O = KC // HD
    PG = QC // KC
    FT = w_gate.shape[1] // HD
    assert n >= O and n % 2 == 0 and FT % O == 0 and PG <= 16
    FO = FT // O
    F0 = FO // 2
    F1 = FO - F0
    QG = PG * HD
    G3 = QG + 2 * HD
    W0, W1 = F0 * HD, F1 * HD
    assert W1 <= QG
    reuse = W1 <= Dl <= G3
    c = dict(n=n, T=T, O=O, S=S, Dl=Dl, L=L, PG=PG, FO=FO, F0=F0, F1=F1, reuse=reuse)
    half = np.arange(HD) % (HD // 2)
    freq = jnp.asarray((rope_base ** (-half * 2.0 / HD)).astype(np.float32)[None, :])
    dma = pltpu.SemaphoreType.DMA
    V = pltpu.VMEM
    anywhere = pl.BlockSpec(memory_space=pl.ANY)
    vmem = pl.BlockSpec(memory_space=pltpu.VMEM)
    packed = pl.pallas_call(
        functools.partial(layer_kernel, c),
        out_shape=pltpu.VMEM((S, Dl + 2 * KC), BF),
        in_specs=[anywhere] * 14,
        out_specs=vmem,
        scratch_shapes=[
            pltpu.SMEM(lengths.shape, jnp.int32),
            V((S, Dl), BF),
            V((1, Dl), F32),
            V((1, Dl), F32),
            V((1, HD), F32),
            V((O, Dl, G3), BF),
            V((1, 16, HD) if reuse else (O, W1, Dl), BF),
            V((QC, Dl), BF),
            V((Dl, FT * HD), BF),
            V((Dl, FT * HD), BF),
            V(key_cache.shape, BF),
            V(value_cache.shape, BF),
            V((O, S, G3 + HD), BF),
            V((T, n, S, G3 + HD), BF),
            V((T, S, QG), BF),
            V((T, S, 2 * HD), BF),
            V((T, S, HD), F32),
            V((O, S, QG), BF),
            V((O, S, 2 * HD), BF),
            V((O, S, QG + HD), BF),
            V((T, n, S, QG + HD), BF),
            V((T, S, QG), BF),
            V((O, S, QG), BF),
            V((T, S, Dl), F32),
            V((O, S, 2 * W0 + HD), BF),
            V((O, S, 2 * W1), BF),
            V((T, n, S, 2 * W0 + HD), BF),
            V((T, n, S, 2 * W1), BF),
            V((T, S, W0), BF),
            V((T, S, W1), BF),
            V((O, S, W0), BF),
            V((O, S, W1), BF),
            V((T, S, Dl), F32),
            dma((5,)),
            dma((5,)),
            dma((O, 2)),
            dma((2,)),
            dma,
            dma((T,)),
            dma((T,)),
            dma((O,)),
            dma((T,)),
            dma,
            dma,
            dma((T,)),
            dma((T,)),
            dma((O,)),
            dma((T - 1,)),
            dma((T - 1,)),
            dma((2,)),
            dma((T, 2)),
            dma((2, T)),
            dma((O, 2)),
            dma((T - 1,)),
            dma((T - 1,)),
        ],
        compiler_params=pltpu.CompilerParams(
            collective_id=0, has_side_effects=True, vmem_limit_bytes=67000000
        ),
    )(
        lengths,
        hidden,
        gain_in[None, :],
        gain_post[None, :],
        freq,
        key_cache,
        value_cache,
        w_query,
        w_key,
        w_value,
        w_output,
        w_gate,
        w_up,
        w_down,
    )
    return pl.pallas_call(
        split_kernel,
        out_shape=(
            jax.ShapeDtypeStruct((S, Dl), BF),
            jax.ShapeDtypeStruct((S, KC), BF),
            jax.ShapeDtypeStruct((S, KC), BF),
        ),
        in_specs=[vmem],
        out_specs=(vmem,) * 3,
    )(pltpu.with_memory_space_constraint(packed, pltpu.VMEM))


def solution(mesh):
    placed = (
        P("groups", "kvseq"),
        P("groups"),
        P("groups", "kvseq", "tensor"),
        P("groups", "kvseq", "tensor"),
        P("kvseq"),
        P("kvseq", "tensor"),
        P("kvseq", "tensor"),
        P("kvseq", "tensor"),
        P("tensor", "kvseq"),
        P("kvseq"),
        P("kvseq", "tensor"),
        P("kvseq", "tensor"),
        P("tensor", "kvseq"),
    )
    return jax.shard_map(
        functools.partial(per_device, mesh.shape["kvseq"], mesh.shape["tensor"]),
        mesh=mesh,
        in_specs=placed,
        out_specs=(P("groups", "kvseq"), P("groups", "tensor"), P("groups", "tensor")),
        check_vma=False,
    )
```

```python
import functools

import jax
import jax.numpy as jnp
import numpy as np
from jax import lax
from jax.experimental import pallas as pl
from jax.experimental.pallas import tpu as pltpu
from jax.sharding import PartitionSpec as P

HD = 128
epsilon = 1e-06
ATTEND_ORDER = (0, 3, 2, 1)
rope_base = 1000000.0
BF = jnp.bfloat16
F32 = jnp.float32
MESH = pl.DeviceIdType.MESH


def mult(x, m):
    return pl.multiple_of(x, m)


def accumulate(n, load, op=jnp.add):
    u = 8 if n % 8 == 0 else 1

    def group(first, acc):
        for j in range(u):
            x = load(first + j)
            acc = x if acc is None else jax.tree.map(op, acc, x)
        return acc

    acc = group(0, None)
    if n == u:
        return acc
    return lax.fori_loop(1, n // u, lambda i, a: group(i * u, a), acc)


def split_kernel(packed, out, new_keys, new_values):
    Dl, KC = out.shape[1], new_keys.shape[1]
    out[...] = packed[:, :Dl]
    new_keys[...] = packed[:, Dl : Dl + KC]
    new_values[...] = packed[:, Dl + KC :]


def layer_kernel(
    c,
    lengths_hbm,
    hidden_hbm,
    gain_in_hbm,
    gain_post_hbm,
    freq_hbm,
    kc_hbm,
    vc_hbm,
    wq_hbm,
    wk_hbm,
    wv_hbm,
    wo_hbm,
    wg_hbm,
    wu_hbm,
    wd_hbm,
    out,
    lengths,
    hidden,
    gain_in,
    gain_post,
    freq,
    wqkv,
    tail,
    wo,
    wg,
    wu,
    kc,
    vc,
    send_a,
    recv_a,
    qg,
    kvg,
    own_scores,
    all_q,
    all_kv,
    send_b,
    recv_b,
    ab,
    all_b,
    part_1,
    send_c0,
    send_c1,
    recv_c0,
    recv_c1,
    ic0,
    ic1,
    all_c0,
    all_c1,
    part_2,
    ssem,
    wsem,
    fsem,
    dsem,
    sa_s,
    sa_r,
    ga_s,
    ga_r,
    gk_s,
    gk_r,
    sb_s,
    sb_r,
    gb_s,
    gb_r,
    t1_s,
    t1_r,
    sc_s,
    sc_r,
    gc_s,
    gc_r,
    t2_s,
    t2_r,
):
    n, T, O = c["n"], c["T"], c["O"]
    S, Dl, L = c["S"], c["Dl"], c["L"]
    PG, FO, F0, F1 = c["PG"], c["FO"], c["F0"], c["F1"]
    QG = PG * HD
    G3 = QG + 2 * HD
    KC = O * HD
    W0, W1 = F0 * HD, F1 * HD
    D = float(Dl * n)
    base = (n - O) // 2
    me = lax.axis_index("kvseq")
    t = lax.axis_index("tensor")
    owner = (me >= base) & (me < base + O) & (t == T - 1)
    o_me = me - base
    half_n = n // 2
    side = me // half_n

    def mine(o):
        return (me == base + o) & (t == T - 1)

    def order(k):
        if O != 4:
            return lax.rem(me + k, O)
        oz = (side + 1 + k // 2) % 2
        oy = (me + 1 + k % 2) % 2
        return oz * 2 + oy

    def near(k):
        return order(O - 1 - k)

    def local(src, dst, sem):
        return pltpu.make_async_copy(src, dst, sem)

    small = [
        local(hidden_hbm, hidden, ssem.at[0]),
        local(gain_in_hbm, gain_in, ssem.at[1]),
        local(lengths_hbm, lengths, ssem.at[2]),
        local(freq_hbm, freq, ssem.at[3]),
        local(gain_post_hbm, gain_post, ssem.at[4]),
    ]
    half = Dl // 2

    def first(k):
        o = order(k)
        return [
            [
                local(
                    src.at[pl.ds(b * half, half), pl.ds(mult(o * width, HD), width)],
                    wqkv.at[k, pl.ds(b * half, half), pl.ds(at, width)],
                    fsem.at[k, b],
                )
                for src, at, width in (
                    (wq_hbm, 0, QG),
                    (wk_hbm, QG, HD),
                    (wv_hbm, QG + HD, HD),
                )
            ]
            for b in range(2)
        ]

    firsts = [first(k) for k in range(O)]

    def first_wait(k, b):
        rows = pl.ds(b * half, half)
        local(wq_hbm.at[rows, pl.ds(0, G3)], wqkv.at[k, rows, :], fsem.at[k, b]).wait()

    kv_copies = [local(kc_hbm, kc, wsem.at[0]), local(vc_hbm, vc, wsem.at[1])]
    later = [
        local(wo_hbm, wo, wsem.at[2]),
        local(wg_hbm, wg, wsem.at[3]),
        local(wu_hbm, wu, wsem.at[4]),
    ]

    def down_0(o):
        return wo.at[pl.ds(mult(o * QG, HD), W0), :]

    def down_1(o):
        return wqkv.at[o, pl.ds(0, W1), pl.ds(0, Dl)] if c["reuse"] else tail.at[o]

    downs_0 = [
        local(wd_hbm.at[pl.ds(o * FO * HD, W0), :], down_0(o), dsem.at[0]) for o in range(O)
    ]
    downs_1 = [
        local(wd_hbm.at[pl.ds((o * FO + F0) * HD, W1), :], down_1(o), dsem.at[1])
        for o in range(O)
    ]
    for x in small:
        x.start()
    for k in range(O):
        for b in range(2):
            for x in firsts[k][b]:
                x.start(priority=1)

    barrier = pltpu.get_barrier_semaphore()
    for dt in range(T):

        def greet(k, _):
            pl.semaphore_signal(
                barrier,
                inc=1,
                device_id={"kvseq": lax.rem(me + k, n), "tensor": lax.rem(t + dt, T)},
                device_id_type=MESH,
            )
            return 0

        lax.fori_loop(0 if dt else 1, n, greet, 0)

    def remote(src, dst, s_sem, r_sem, k, tt):
        return pltpu.make_async_remote_copy(
            src_ref=src, dst_ref=dst, send_sem=s_sem, recv_sem=r_sem,
            device_id={"kvseq": k, "tensor": tt}, device_id_type=MESH,
        )

    def to_owner(src, recv, s_sem, r_sem, o):
        return remote(src, recv, s_sem, r_sem, base + o, T - 1)

    def scatter(src, dst, s_sem, r_sem, o):
        @pl.when(jnp.logical_not(mine(o)))
        def _():
            to_owner(src, dst, s_sem, r_sem, o).start()

        @pl.when(mine(o))
        def _():
            dst[...] = src[...]

    def scatter_wait_send(send, s_sem):
        @pl.when(jnp.logical_not(owner))
        def _():
            remote(send, send, s_sem, s_sem, me, t).wait_send()

        @pl.when(owner)
        def _():
            x = send.at[pl.ds(0, O - 1)]
            remote(x, x, s_sem, s_sem, me, t).wait_send()

    def arrivals(tt):
        return pl.ds(0, n - 1 if tt == T - 1 else n)

    def owner_wait(recv, r_sem, tt):
        x = recv.at[tt, arrivals(tt)]
        remote(x, x, sa_s, r_sem, me, tt).wait_recv()

    def each_target(f):
        def cross(k, _):
            f(k + (1 - side) * (n - 1 - 2 * k))
            return 0

        def same(k, _):
            f(k + side * (n - 1 - 2 * k))
            return 0

        lax.fori_loop(0, half_n, cross, 0)
        lax.fori_loop(0, n - half_n, same, 0)

    def spread(src, dst, s_sem, r_sem, tt, rising=False):
        def one(d):
            def send():
                remote(src, dst, s_sem.at[tt], r_sem, d, tt).start()

            if tt == T - 1:
                pl.when(d != me)(send)
            else:
                send()

        if rising:
            lax.fori_loop(0, n, lambda d, _: (one(d), 0)[1], 0)
        else:
            each_target(one)
        if tt == T - 1:
            dst[...] = src[...]

    def spread_wait_send(like, width, s_sem, tt):
        x = like.at[tt, arrivals(tt), :, pl.ds(0, width)]
        remote(x, x, s_sem.at[tt], s_sem.at[tt], me, tt).wait_send()

    def spread_wait(dst, s_sem, r_sem, o):
        @pl.when(jnp.logical_not(mine(o)))
        def _():
            remote(dst, dst, s_sem.at[0], r_sem, base + o, T - 1).wait_recv()

    def pair_copies(part, s_sem, r_sem):
        return [
            remote(
                part.at[t], part.at[t], s_sem.at[k - 1], r_sem.at[k - 1], me, lax.rem(t + k, T)
            )
            for k in range(1, T)
        ]

    def pair_sum(part, s_sem, r_sem):
        for x in pair_copies(part, s_sem, r_sem):
            x.start()
        for k in range(1, T):
            src = lax.rem(t + T - k, T)
            x = part.at[src]
            remote(x, x, s_sem.at[k - 1], r_sem.at[k - 1], me, src).wait_recv()
        total = part[0]
        for i in range(1, T):
            total = total + part[i]
        return total

    lane = lax.broadcasted_iota(jnp.int32, (S, HD), 1)
    row = lax.broadcasted_iota(jnp.int32, (S, HD), 0)

    def squares_block(x):
        s = jnp.broadcast_to(jnp.sum(x * x, axis=1, keepdims=True), (S, HD))
        high = s.astype(BF).astype(F32)
        return jnp.where(lane < HD // 2, high, s - high).astype(BF)

    def row_scale(block):
        total = jnp.sum(block, axis=1, keepdims=True) * (2.0 / HD)
        return lax.rsqrt(total / D + epsilon)

    small[0].wait()
    small[1].wait()
    stream = hidden[...].astype(F32)
    xg = (stream * gain_in[...]).astype(BF)
    sq = squares_block(stream)

    for k in range(O):
        o = order(k)
        first_wait(k, 0)
        part = jnp.dot(xg[:, :half], wqkv[k, :half, :], preferred_element_type=F32)
        first_wait(k, 1)
        if k == max(O - 2, 0):
            for x in kv_copies:
                x.start(priority=1)
        part = part + jnp.dot(xg[:, half:], wqkv[k, half:, :], preferred_element_type=F32)
        send_a[k, :, :G3] = part.astype(BF)
        send_a[k, :, G3:] = sq
        if k == 0:
            pl.semaphore_wait(barrier, n * T - 1)
        scatter(send_a.at[k], recv_a.at[t, me], sa_s, sa_r.at[t], o)
    for x in later + downs_1:
        x.start(priority=1)

    small[2].wait()
    small[3].wait()
    position = jnp.zeros((S, HD), F32)
    for s in range(S):
        position = jnp.where(row == s, lengths[s].astype(F32), position)
    angle = position * freq[...]
    cosine = jnp.cos(angle)
    sine = jnp.sin(angle)
    sine = jnp.where(lane < HD // 2, -sine, sine)
    factor = float(HD) ** (-0.5)

    @pl.when(owner)
    def _():
        scale = None
        for tt in reversed(range(T)):
            owner_wait(recv_a, sa_r.at[tt], tt)
            total = accumulate(n, lambda k: recv_a[tt, k].astype(F32))
            if scale is None:
                scale = row_scale(total[:, G3:])
            for j in range(PG + 1):
                v = total[:, j * HD : (j + 1) * HD]
                v = ((v * cosine + pltpu.roll(v, HD // 2, 1) * sine) * scale).astype(BF)
                if j < PG:
                    qg[tt, :, j * HD : (j + 1) * HD] = v
                else:
                    kvg[tt, :, :HD] = v
            kvg[tt, :, HD:] = (total[:, QG + HD : G3] * scale).astype(BF)
            spread(qg.at[tt], all_q.at[o_me], ga_s, ga_r.at[o_me], tt)
        for tt in range(T):
            key = kvg[tt, :, :HD].astype(F32)
            block = jnp.zeros((S, HD), F32)
            for j in range(PG):
                q = qg[tt, :, j * HD : (j + 1) * HD].astype(F32)
                block = jnp.where(
                    lane == j, jnp.sum(q * key, axis=1, keepdims=True) * factor, block
                )
            own_scores[tt] = block

    R = PG * S
    brow = lax.broadcasted_iota(jnp.int32, (R, L), 0) % S
    orow = lax.broadcasted_iota(jnp.int32, (R, HD), 0) % S
    limit = jnp.zeros((R, L), jnp.int32)
    for s in range(S):
        limit = jnp.where(brow == s, lengths[s], limit)
    place = lax.broadcasted_iota(jnp.int32, (R, L), 1) + me * L
    valid = place < limit
    for x in kv_copies:
        x.wait()
    group = lane % 16
    third = (lane % (HD // 2)) // 16

    def attend_one(g):
        q = jnp.concatenate(
            [all_q[g, :, j * HD : (j + 1) * HD].astype(F32) for j in range(PG)], axis=0
        ).astype(BF)
        cols = pl.ds(mult(g * HD, HD), HD)
        scores = jnp.zeros((R, L), F32)
        for s in range(S):
            x = lax.dot_general(
                q, kc[s, :, cols], (((1,), (1,)), ((), ())), preferred_element_type=F32
            )
            scores = jnp.where(brow == s, x, scores)
        scores = jnp.where(valid, scores * factor, -1e30)
        top = jnp.max(scores, axis=1, keepdims=True)
        w = jnp.where(valid, jnp.exp(scores - top), 0.0)
        total = jnp.sum(w, axis=1, keepdims=True)
        w = w.astype(BF)
        mixed = jnp.zeros((R, HD), F32)
        for s in range(S):
            x = jnp.dot(w, vc[s, :, cols], preferred_element_type=F32)
            mixed = jnp.where(orow == s, x, mixed)
        ml = jnp.zeros((S, HD), F32)
        for j in range(PG):
            rows = slice(j * S, (j + 1) * S)
            send_b[g, :, j * HD : (j + 1) * HD] = mixed[rows].astype(BF)
            ml = jnp.where(group == j, jnp.where(lane < HD // 2, top[rows], total[rows]), ml)
        high = ml.astype(BF).astype(F32)
        rest = ml - high
        middle = rest.astype(BF).astype(F32)
        low = rest - middle
        parts = jnp.where(third == 0, high, jnp.where(third == 1, middle, low))
        send_b[g, :, QG:] = parts.astype(BF)

    def attend(i, _):
        k = i
        if O == len(ATTEND_ORDER):
            for j, v in enumerate(ATTEND_ORDER):
                k = jnp.where(i == j, v, k)
        g = near(k)
        spread_wait(all_q.at[g], ga_s, ga_r.at[g], g)
        attend_one(g)
        scatter(send_b.at[g], recv_b.at[t, me], sb_s, sb_r.at[t], g)
        return 0

    lax.fori_loop(0, O, attend, 0)

    @pl.when(owner)
    def _():
        for tt in reversed(range(T)):
            owner_wait(recv_b, sb_r.at[tt], tt)

            def stats(k):
                x = recv_b[tt, k, :, QG:].astype(F32)
                return x + pltpu.roll(x, HD - 16, 1) + pltpu.roll(x, HD - 32, 1)

            if n <= 8:
                known = [stats(k) for k in range(n)]
                stats = known.__getitem__
            top = accumulate(n, stats, jnp.maximum)
            total = accumulate(
                n, lambda k: pltpu.roll(stats(k), HD // 2, 1) * jnp.exp(stats(k) - top)
            )
            own = own_scores[tt]
            best = jnp.maximum(top, own)
            old_scale = jnp.exp(top - best)
            own_weight = jnp.exp(own - best)
            bottom = total * old_scale + own_weight
            old_scale = old_scale / bottom
            own_weight = own_weight / bottom

            def weighted(k):
                scale = jnp.exp(stats(k) - top) * old_scale
                return tuple(
                    recv_b[tt, k, :, j * HD : (j + 1) * HD].astype(F32) * scale[:, j : j + 1]
                    for j in range(PG)
                )

            mixed = accumulate(n, weighted)
            val = kvg[tt, :, HD:].astype(F32)
            for j in range(PG):
                res = mixed[j] + own_weight[:, j : j + 1] * val
                ab[tt, :, j * HD : (j + 1) * HD] = res.astype(BF)
            spread(ab.at[tt], all_b.at[o_me], gb_s, gb_r.at[o_me], tt)
        for tt in range(T):
            spread(kvg.at[tt], all_kv.at[o_me], gk_s, gk_r, tt)

    later[0].wait()

    def output_block(i, acc):
        g = near(i)
        spread_wait(all_b.at[g], gb_s, gb_r.at[g], g)
        w = wo[pl.ds(mult(g * QG, HD), QG), :]
        return acc + jnp.dot(all_b[g], w, preferred_element_type=F32)

    part_1[t] = lax.fori_loop(0, O, output_block, jnp.zeros((S, Dl), F32))
    for x in downs_0:
        x.start(priority=1)
    small[4].wait()
    residual = hidden[...].astype(F32) + pair_sum(part_1, t1_s, t1_r)
    sq_post = squares_block(residual)
    rg = (residual * gain_post[...]).astype(BF)
    later[1].wait()
    later[2].wait()

    def widen(k, _):
        o = order(k)
        for send, recv, i, at, W in (
            (send_c0, recv_c0, 0, 0, W0),
            (send_c1, recv_c1, 1, F0, W1),
        ):
            begin = (o * FO + at) * HD
            for b, w in enumerate((wg, wu)):
                for j in range(0, W, 256):
                    step = min(256, W - j)
                    x = jnp.dot(
                        rg, w[:, pl.ds(mult(begin + j, HD), step)], preferred_element_type=F32
                    )
                    send[o, :, b * W + j : b * W + j + step] = x.astype(BF)
            if i == 0:
                send[o, :, 2 * W :] = sq_post
            scatter(send.at[o], recv.at[t, me], sc_s.at[i], sc_r.at[t, i], o)
        return 0

    lax.fori_loop(0, O, widen, 0)

    @pl.when(jnp.logical_not(owner))
    def _():
        remote(all_kv, all_kv, gk_s.at[0], gk_r, me, t).wait_recv()

    @pl.when(owner)
    def _():
        x = all_kv.at[pl.ds(0, O - 1)]
        remote(x, x, gk_s.at[0], gk_r, me, t).wait_recv()

    for g in range(O):
        out[:, Dl + g * HD : Dl + (g + 1) * HD] = all_kv[g, :, :HD]
        out[:, Dl + KC + g * HD : Dl + KC + (g + 1) * HD] = all_kv[g, :, HD:]

    @pl.when(owner)
    def _():
        scales = [None] * T
        for i, recv, ic, all_c, W in ((0, recv_c0, ic0, all_c0, W0), (1, recv_c1, ic1, all_c1, W1)):
            for tt in range(T):
                owner_wait(recv, sc_r.at[tt, i], tt)
                if i == 0:
                    scales[tt] = row_scale(
                        accumulate(n, lambda k: recv[tt, k, :, 2 * W :].astype(F32))
                    )
                for j in range(0, W, HD):
                    gate = accumulate(n, lambda k: recv[tt, k, :, j : j + HD].astype(F32))
                    up = accumulate(n, lambda k: recv[tt, k, :, W + j : W + j + HD].astype(F32))
                    gate = gate * scales[tt]
                    up = up * scales[tt]
                    ic[tt, :, j : j + HD] = (gate * jax.nn.sigmoid(gate) * up).astype(BF)
                spread(ic.at[tt], all_c.at[o_me], gc_s.at[i], gc_r.at[o_me, i], tt, rising=True)

    for i, W in ((0, W0), (1, W1)):
        rows = pl.ds(0, O * W)
        local(wd_hbm.at[rows, :], wo.at[rows, :], dsem.at[i]).wait()

    def down_block(k, acc):
        o = near(k)
        spread_wait(all_c0.at[o], gc_s.at[0], gc_r.at[o, 0], o)
        acc = acc + jnp.dot(all_c0[o], down_0(o)[...], preferred_element_type=F32)
        spread_wait(all_c1.at[o], gc_s.at[1], gc_r.at[o, 1], o)
        return acc + jnp.dot(all_c1[o], down_1(o)[...], preferred_element_type=F32)

    part_2[t] = lax.fori_loop(0, O, down_block, jnp.zeros((S, Dl), F32))
    out[:, :Dl] = (residual + pair_sum(part_2, t2_s, t2_r)).astype(BF)

    for send, s_sem in (
        (send_a, sa_s),
        (send_b, sb_s),
        (send_c0, sc_s.at[0]),
        (send_c1, sc_s.at[1]),
    ):
        scatter_wait_send(send, s_sem)

    @pl.when(owner)
    def _():
        for tt in range(T):
            spread_wait_send(recv_b, QG, ga_s, tt)
            spread_wait_send(recv_b, 2 * HD, gk_s, tt)
            spread_wait_send(recv_b, QG, gb_s, tt)
            spread_wait_send(recv_c0, W0, gc_s.at[0], tt)
            spread_wait_send(recv_c1, W1, gc_s.at[1], tt)

    for part, s_sem, r_sem in ((part_1, t1_s, t1_r), (part_2, t2_s, t2_r)):
        for x in pair_copies(part, s_sem, r_sem):
            x.wait_send()


def per_device(
    n,
    T,
    hidden,
    lengths,
    key_cache,
    value_cache,
    gain_in,
    w_query,
    w_key,
    w_value,
    w_output,
    gain_post,
    w_gate,
    w_up,
    w_down,
):
    S, Dl = hidden.shape
    L = key_cache.shape[1]
    QC, KC = w_query.shape[1], w_key.shape[1]
    O = KC // HD
    PG = QC // KC
    FT = w_gate.shape[1] // HD
    assert n >= O and n % 2 == 0 and FT % O == 0 and PG <= 16
    FO = FT // O
    F0 = FO // 2
    F1 = FO - F0
    QG = PG * HD
    G3 = QG + 2 * HD
    W0, W1 = F0 * HD, F1 * HD
    assert W1 <= QG
    reuse = W1 <= Dl <= G3
    c = dict(n=n, T=T, O=O, S=S, Dl=Dl, L=L, PG=PG, FO=FO, F0=F0, F1=F1, reuse=reuse)
    half = np.arange(HD) % (HD // 2)
    freq = jnp.asarray((rope_base ** (-half * 2.0 / HD)).astype(np.float32)[None, :])
    dma = pltpu.SemaphoreType.DMA
    V = pltpu.VMEM
    anywhere = pl.BlockSpec(memory_space=pl.ANY)
    vmem = pl.BlockSpec(memory_space=pltpu.VMEM)
    packed = pl.pallas_call(
        functools.partial(layer_kernel, c),
        out_shape=pltpu.VMEM((S, Dl + 2 * KC), BF),
        in_specs=[anywhere] * 14,
        out_specs=vmem,
        scratch_shapes=[
            pltpu.SMEM(lengths.shape, jnp.int32),
            V((S, Dl), BF),
            V((1, Dl), F32),
            V((1, Dl), F32),
            V((1, HD), F32),
            V((O, Dl, G3), BF),
            V((1, 16, HD) if reuse else (O, W1, Dl), BF),
            V((QC, Dl), BF),
            V((Dl, FT * HD), BF),
            V((Dl, FT * HD), BF),
            V(key_cache.shape, BF),
            V(value_cache.shape, BF),
            V((O, S, G3 + HD), BF),
            V((T, n, S, G3 + HD), BF),
            V((T, S, QG), BF),
            V((T, S, 2 * HD), BF),
            V((T, S, HD), F32),
            V((O, S, QG), BF),
            V((O, S, 2 * HD), BF),
            V((O, S, QG + HD), BF),
            V((T, n, S, QG + HD), BF),
            V((T, S, QG), BF),
            V((O, S, QG), BF),
            V((T, S, Dl), F32),
            V((O, S, 2 * W0 + HD), BF),
            V((O, S, 2 * W1), BF),
            V((T, n, S, 2 * W0 + HD), BF),
            V((T, n, S, 2 * W1), BF),
            V((T, S, W0), BF),
            V((T, S, W1), BF),
            V((O, S, W0), BF),
            V((O, S, W1), BF),
            V((T, S, Dl), F32),
            dma((5,)),
            dma((5,)),
            dma((O, 2)),
            dma((2,)),
            dma,
            dma((T,)),
            dma((T,)),
            dma((O,)),
            dma((T,)),
            dma,
            dma,
            dma((T,)),
            dma((T,)),
            dma((O,)),
            dma((T - 1,)),
            dma((T - 1,)),
            dma((2,)),
            dma((T, 2)),
            dma((2, T)),
            dma((O, 2)),
            dma((T - 1,)),
            dma((T - 1,)),
        ],
        compiler_params=pltpu.CompilerParams(
            collective_id=0, has_side_effects=True, vmem_limit_bytes=67000000
        ),
    )(
        lengths,
        hidden,
        gain_in[None, :],
        gain_post[None, :],
        freq,
        key_cache,
        value_cache,
        w_query,
        w_key,
        w_value,
        w_output,
        w_gate,
        w_up,
        w_down,
    )
    return pl.pallas_call(
        split_kernel,
        out_shape=(
            jax.ShapeDtypeStruct((S, Dl), BF),
            jax.ShapeDtypeStruct((S, KC), BF),
            jax.ShapeDtypeStruct((S, KC), BF),
        ),
        in_specs=[vmem],
        out_specs=(vmem,) * 3,
    )(pltpu.with_memory_space_constraint(packed, pltpu.VMEM))


def solution(mesh):
    placed = (
        P("groups", "kvseq"),
        P("groups"),
        P("groups", "kvseq", "tensor"),
        P("groups", "kvseq", "tensor"),
        P("kvseq"),
        P("kvseq", "tensor"),
        P("kvseq", "tensor"),
        P("kvseq", "tensor"),
        P("tensor", "kvseq"),
        P("kvseq"),
        P("kvseq", "tensor"),
        P("kvseq", "tensor"),
        P("tensor", "kvseq"),
    )
    return jax.shard_map(
        functools.partial(per_device, mesh.shape["kvseq"], mesh.shape["tensor"]),
        mesh=mesh,
        in_specs=placed,
        out_specs=(P("groups", "kvseq"), P("groups", "tensor"), P("groups", "tensor")),
        check_vma=False,
    )
```
